8 devices in a mesh: rep: 1 (over z), r: 2 (over y), s: 4 (over x, core).
Axes of the slice: x: 2, y: 2, z: 1, core: 2. Of those that a mesh axis runs over, the one named last changes fastest.
Arguments:
- x: bfloat16 [8, 4096, 1024], P(('rep', 'r', 's'))
- dy: bfloat16 [8, 4096, 1024], P(('rep', 'r', 's'))
- w_gate: bfloat16 [2, 1024, 2560], P(None, 's')
- w_up: bfloat16 [2, 1024, 2560], P(None, 's')
- w_down: bfloat16 [2, 2560, 1024], P(None, 's')
- m_w_gate: float32 [2, 1024, 2560], P(None, 's')
- m_w_up: float32 [2, 1024, 2560], P(None, 's')
- m_w_down: float32 [2, 2560, 1024], P(None, 's')
- v_w_gate: float32 [2, 1024, 2560], P(None, 's')
- v_w_up: float32 [2, 1024, 2560], P(None, 's')
- v_w_down: float32 [2, 2560, 1024], P(None, 's')
Outputs:
- output 1: bfloat16 [2, 1024, 2560], P('rep', 's')
- output 2: bfloat16 [2, 1024, 2560], P('rep', 's')
- output 3: bfloat16 [2, 2560, 1024], P('rep', 's')
- output 4: float32 [2, 1024, 2560], P('rep', 's')
- output 5: float32 [2, 1024, 2560], P('rep', 's')
- output 6: float32 [2, 2560, 1024], P('rep', 's')
- output 7: float32 [2, 1024, 2560], P('rep', 's')
- output 8: float32 [2, 1024, 2560], P('rep', 's')
- output 9: float32 [2, 2560, 1024], P('rep', 's')
All inputs are finite; a program needn't handle non-finite values.
Results may differ from the reference program's by a relative error of at most 0.022.
Values are sent between devices in bfloat16 or wider.
A program may use at most 2 GiB of HBM per device.

```python
import jax
import jax.numpy as jnp
from jax import lax

SEQUENCES = 8
TOKENS = 4096
D = 1024
FF = 2560
LAYERS = 2
NAMES = ("w_gate", "w_up", "w_down")
SHAPES = {"w_gate": (LAYERS, D, FF), "w_up": (LAYERS, D, FF), "w_down": (LAYERS, FF, D)}


def bump(key, n, height):
    away = (jnp.arange(n, dtype=jnp.int32) - jax.random.randint(key, (), 0, n, jnp.int32)) % n
    return jnp.where(away < n // 8, height, 1.0)


def together(key, own, strength):
    shared = jax.random.normal(key, own.shape[1:], jnp.float32)
    return (own + strength * shared) * lax.rsqrt(1 + strength * strength)


def setup_inputs(seed: int = 0, part: int = 0) -> dict:
    kx, kdy, ka, kb, kz, kf, kh, kl, *keys = jax.random.split(jax.random.key(seed), 8 + 3 * len(NAMES))
    kx, kdy, ka, kb = (jax.random.fold_in(k, part) for k in (kx, kdy, ka, kb))
    kw, km, kv = (keys[i::3] for i in range(3))
    shape = (SEQUENCES, TOKENS, D)
    much_x, much_dy = jax.random.uniform(kz, (2,), jnp.float32, 0.0, 1.0)
    loud = 2.0 ** jax.random.uniform(jax.random.fold_in(kz, 1), (), jnp.float32, -1.0, 2.0)
    layers = 2.0 ** jax.random.uniform(kl, (LAYERS, 1, 1), jnp.float32, -1.0, 1.0)
    x = together(ka, jax.random.normal(kx, shape, jnp.float32), much_x) * bump(kf, D, 4.0)
    dy = together(kb, jax.random.normal(kdy, shape, jnp.float32), much_dy)
    drawn = {"x": x.astype(jnp.bfloat16), "dy": (loud * dy * (SEQUENCES * TOKENS) ** -0.5).astype(jnp.bfloat16)}
    for key, name in zip(kw, NAMES, strict=True):
        w = jax.random.normal(key, SHAPES[name], jnp.float32) * SHAPES[name][1] ** -0.5
        drawn[name] = (w * {"w_gate": 1.0, "w_up": bump(kh, FF, 4.0), "w_down": layers}[name]).astype(jnp.bfloat16)
    for key, name in zip(km, NAMES, strict=True):
        drawn[f"m_{name}"] = 0.1 * jax.random.normal(key, SHAPES[name], jnp.float32)
    for key, name in zip(kv, NAMES, strict=True):
        drawn[f"v_{name}"] = jax.random.uniform(key, SHAPES[name], jnp.float32, 0.005, 0.015)
    return drawn


def matmul(a, w):
    return jnp.dot(a, w, preferred_element_type=jnp.float32).astype(jnp.bfloat16)


def normed(h):
    wide = h.astype(jnp.float32)
    scale = lax.rsqrt(jnp.mean(wide**2, -1, keepdims=True) + 1e-6)
    return (wide * scale).astype(jnp.bfloat16)


def layer(h, w):
    a = normed(h)
    gate = jnp.dot(a, w["w_gate"], preferred_element_type=jnp.float32)
    up = jnp.dot(a, w["w_up"], preferred_element_type=jnp.float32)
    return h + matmul((jax.nn.silu(gate) * up).astype(jnp.bfloat16), w["w_down"])


def adamw(w, m, v, g):
    m = 0.9 * m + 0.1 * g
    v = 0.95 * v + 0.05 * g * g
    step = m * lax.rsqrt(v + 1e-8) + 0.1 * w
    return (w - 0.02 * step).astype(jnp.bfloat16), m, v


def clipped(gradients, sum_of_squares, count):
    factor = jnp.minimum(1.0, 0.5 * lax.rsqrt(sum_of_squares / count + 1e-30))
    return [g * factor for g in gradients]


def stack(weights, h):
    return lax.scan(lambda h, w: (layer(h, w), None), h, weights)[0]


def reference(x, dy, w_gate, w_up, w_down, m_w_gate, m_w_up, m_w_down, v_w_gate, v_w_up, v_w_down):
    weights = dict(zip(NAMES, (w_gate, w_up, w_down), strict=True))

    def take(so_far, sequence):
        h, by_y = sequence
        _, back = jax.vjp(lambda w: stack(w, h), weights)
        return jax.tree.map(lambda total, term: total + term.astype(jnp.float32), so_far, back(by_y)[0]), None

    none_yet = {name: jnp.zeros(w.shape, jnp.float32) for name, w in weights.items()}
    by_weights, _ = lax.scan(take, none_yet, (x, dy))
    gradients = [by_weights[name].astype(jnp.bfloat16).astype(jnp.float32) for name in NAMES]
    gradients = clipped(gradients, sum(jnp.sum(g * g) for g in gradients), sum(g.size for g in gradients))
    new = [
        adamw(w.astype(jnp.float32), m, v, g)
        for w, m, v, g in zip((w_gate, w_up, w_down), (m_w_gate, m_w_up, m_w_down), (v_w_gate, v_w_up, v_w_down), gradients, strict=True)
    ]
    return tuple(one[which] for which in range(3) for one in new)
```

```python
import functools

import jax
import jax.numpy as jnp
from jax import lax
from jax.experimental import pallas as pl
from jax.experimental.pallas import tpu as pltpu
from jax.sharding import PartitionSpec as P

NAMES = ("w_gate", "w_up", "w_down")
TOK, D, FF = 4096, 1024, 2560
NC, CH = 5, 512
bf16, f32 = jnp.bfloat16, jnp.float32
PARAMS = pltpu.CompilerParams(vmem_limit_bytes=62 * 1024 * 1024)


def dot(a, b):
    return jnp.dot(a, b, preferred_element_type=f32)


def dot_nt(a, b):
    return lax.dot_general(a, b, (((1,), (1,)), ((), ())), preferred_element_type=f32)


def dot_tn(a, b):
    return lax.dot_general(a, b, (((0,), (0,)), ((), ())), preferred_element_type=f32)


def cost(products, width, nbytes):
    return pl.CostEstimate(flops=products * 2 * TOK * D * width, bytes_accessed=nbytes, transcendentals=0)


def scale_of(wide):
    return lax.rsqrt(jnp.mean(wide * wide, -1, keepdims=True) + 1e-6)


def sigmoid(g):
    return 0.5 * jnp.tanh(0.5 * g) + 0.5


def once(shape):
    return pl.BlockSpec(shape, lambda *_: (0,) * len(shape), pipeline_mode=pl.Buffered(1))


def forward_up(x, wg, wu, TM=256):
    def body(x_ref, wg_ref, wu_ref, a_ref, g_ref, u_ref, hid_ref):
        wide = x_ref[...].astype(f32)
        a = (wide * scale_of(wide)).astype(bf16)
        a_ref[...] = a
        for n in range(NC):
            c = slice(n * CH, (n + 1) * CH)
            g = dot(a, wg_ref[:, c])
            u = dot(a, wu_ref[:, c])
            g_ref[:, c] = g
            u_ref[:, c] = u
            hid_ref[:, c] = (g * sigmoid(g) * u).astype(bf16)

    row = lambda n: pl.BlockSpec((TM, n), lambda t: (t, 0))
    return pl.pallas_call(
        body,
        grid=(TOK // TM,),
        in_specs=[row(D), once((D, FF)), once((D, FF))],
        out_specs=[row(D), row(FF), row(FF), row(FF)],
        out_shape=[jax.ShapeDtypeStruct((TOK, n), d) for n, d in ((D, bf16), (FF, f32), (FF, f32), (FF, bf16))],
        compiler_params=PARAMS,
        cost_estimate=cost(2, FF, 130_000_000),
        name="forward_up",
    )(x, wg, wu)


def forward_down(x, hid, wd, TM=512):
    def body(x_ref, hid_ref, wd_ref, h_ref, a_ref):
        y = dot(hid_ref[...], wd_ref[...]).astype(bf16)
        h = (x_ref[...].astype(f32) + y.astype(f32)).astype(bf16)
        h_ref[...] = h
        wide = h.astype(f32)
        a_ref[...] = (wide * scale_of(wide)).astype(bf16)

    row = lambda n: pl.BlockSpec((TM, n), lambda t: (t, 0))
    return pl.pallas_call(
        body,
        grid=(TOK // TM,),
        in_specs=[row(D), row(FF), once((FF, D))],
        out_specs=[row(D), row(D)],
        out_shape=[jax.ShapeDtypeStruct((TOK, D), bf16)] * 2,
        compiler_params=PARAMS,
        cost_estimate=cost(1, FF, 60_000_000),
        name="forward_down",
    )(x, hid, wd)


def scatter_out(tmpg, tmpu, tmpd, send_ref, keep_ref):
    me = lax.axis_index("s")
    xx, core = me // 2, me % 2
    for out, oc in ((send_ref, 1 - core), (keep_ref, core)):
        for k, ox in ((0, 1 - xx), (1, xx)):
            o = 2 * ox + oc
            out[k, 0:256, :] = tmpg[o]
            out[k, 256:512, :] = tmpu[o]
            out[k, 512:640, :] = tmpd[o, :, 0:CH]
            out[k, 640:768, :] = tmpd[o, :, CH : 2 * CH]


def products(step, nt, a_v, dy_v, dg_s, du_s, hid_s, tmpg, tmpu, tmpd, send_ref, keep_ref):
    @pl.when(step == nt)
    def _():
        tmpg[...] = dot_tn(a_v[...], dg_s[...]).astype(bf16).reshape(4, 256, CH)

    @pl.when(step == nt + 1)
    def _():
        tmpu[...] = dot_tn(a_v[...], du_s[...]).astype(bf16).reshape(4, 256, CH)

    @pl.when(step == nt + 2)
    def _():
        tmpd[...] = dot_tn(hid_s[...], dy_v[...]).astype(bf16).reshape(4, 128, D)
        scatter_out(tmpg, tmpu, tmpd, send_ref, keep_ref)


def load_tiles(step, nt, TM, pairs, sems):
    copies = lambda i: [pltpu.make_async_copy(src.at[pl.ds(i * TM, TM)], dst.at[pl.ds(i * TM, TM)], sems.at[n, i]) for n, (src, dst) in enumerate(pairs)]

    @pl.when(step == 0)
    def _():
        for i in range(nt):
            for c in copies(i):
                c.start()

    @pl.when(step < nt)
    def _():
        for c in copies(step):
            c.wait()


GRADS = [jax.ShapeDtypeStruct((2, 768, CH), bf16)] * 2
GRAD_SPECS = [pl.BlockSpec((2, 768, CH), lambda t: (0, 0, 0), pipeline_mode=pl.Buffered(1))] * 2
PRODUCT_SCRATCH = (
    [pltpu.VMEM((TOK, D), bf16)] * 2
    + [pltpu.VMEM((TOK, CH), bf16)] * 3
    + [pltpu.VMEM((4, 256, CH), bf16)] * 2
    + [pltpu.VMEM((4, 128, D), bf16)]
)


def backward_top(j, a, dy, wg, wu, wd, TM=512, SUB=256):
    nt = TOK // TM

    def body(a_ref, dy_ref, *rest):
        wgs, wus, wd_ref = rest[0:4], rest[4:8], rest[8]
        dg_ref, du_ref, send_ref, keep_ref, a_v, dy_v, dg_s, du_s, hid_s, tmpg, tmpu, tmpd, wgc, wuc, sems = rest[9:]
        t = pl.program_id(0)
        load_tiles(t, nt, TM, ((a_ref, a_v), (dy_ref, dy_v)), sems)

        @pl.when(t == 0)
        def _():
            wgc[...] = jnp.concatenate([w[...] for w in wgs], axis=1)
            wuc[...] = jnp.concatenate([w[...] for w in wus], axis=1)

        @pl.when(t < nt)
        def _():
            wdc = wd_ref[...].reshape(CH, D)
            for s in range(TM // SUB):
                r = pl.ds(pl.multiple_of(t * TM + s * SUB, SUB), SUB)
                x = a_v[r, :]
                g, u = dot(x, wgc[...]), dot(x, wuc[...])
                dh = dot_nt(dy_v[r, :], wdc).astype(bf16).astype(f32)
                sig = sigmoid(g)
                silu = g * sig
                dg = (dh * u * (sig + silu - silu * sig)).astype(bf16)
                du = (dh * silu).astype(bf16)
                hid_s[r, :] = (silu * u).astype(bf16)
                dg_s[r, :] = dg
                du_s[r, :] = du
                dg_ref[s * SUB : (s + 1) * SUB, :] = dg
                du_ref[s * SUB : (s + 1) * SUB, :] = du

        products(t, nt, a_v, dy_v, dg_s, du_s, hid_s, tmpg, tmpu, tmpd, send_ref, keep_ref)

    col = [pl.BlockSpec((D, 128), functools.partial(lambda q, t: (0, q * NC + j), q), pipeline_mode=pl.Buffered(1)) for q in range(4)]
    tile = pl.BlockSpec((TM, CH), lambda t: (jnp.minimum(t, nt - 1), 0))
    return pl.pallas_call(
        body,
        grid=(nt + 3,),
        in_specs=[pl.BlockSpec(memory_space=pl.ANY)] * 2
        + col
        + col
        + [pl.BlockSpec((4, 128, D), lambda t: (0, j, 0), pipeline_mode=pl.Buffered(1))],
        out_specs=[tile, tile] + GRAD_SPECS,
        out_shape=[jax.ShapeDtypeStruct((TOK, CH), bf16)] * 2 + GRADS,
        scratch_shapes=PRODUCT_SCRATCH + [pltpu.VMEM((D, CH), bf16)] * 2 + [pltpu.SemaphoreType.DMA((2, nt))],
        compiler_params=PARAMS,
        cost_estimate=cost(6, CH, 30_000_000),
        name=f"backward_top_{j}",
    )(a, dy, *[wg] * 4, *[wu] * 4, wd.reshape(4, 640, D))


def backward_through(dgs, dus, wg, wu, h, dy, TM=256):
    def body(*refs):
        dg, du = (jnp.concatenate([refs[5 * i + j][:, 128 * q : 128 * q + 128] for q in range(4) for j in range(NC)], axis=1) for i in range(2))
        wg_ref, wu_ref, h_ref, dy_ref, out_ref = refs[10:]
        da = dot_nt(dg, wg_ref[...]).astype(bf16).astype(f32) + dot_nt(du, wu_ref[...]).astype(bf16).astype(f32)
        da = da.astype(bf16).astype(f32)
        wide = h_ref[...].astype(f32)
        scale = scale_of(wide)
        along = jnp.sum(da * wide, -1, keepdims=True) * (scale * scale * scale * (1.0 / D))
        dh = (da * scale - wide * along).astype(bf16)
        out_ref[...] = (dy_ref[...].astype(f32) + dh.astype(f32)).astype(bf16)

    row = lambda n: pl.BlockSpec((TM, n), lambda t: (t, 0))
    return pl.pallas_call(
        body,
        grid=(TOK // TM,),
        in_specs=[row(CH)] * 10 + [once((D, FF))] * 2 + [row(D)] * 2,
        out_specs=row(D),
        out_shape=jax.ShapeDtypeStruct((TOK, D), bf16),
        compiler_params=PARAMS,
        cost_estimate=cost(2, FF, 80_000_000),
        name="backward_through",
    )(*dgs, *dus, wg, wu, h, dy)


def backward_bottom(j, a, dy, gate, up, wd, TM=512, SUB=256):
    nt = TOK // TM

    def body(a_ref, dy_ref, *rest):
        gs, us, wd_ref = rest[0:4], rest[4:8], rest[8]
        send_ref, keep_ref, a_v, dy_v, dg_s, du_s, hid_s, tmpg, tmpu, tmpd, sems = rest[9:]
        t = pl.program_id(0)
        load_tiles(t, nt, TM, ((a_ref, a_v), (dy_ref, dy_v)), sems)

        @pl.when(t < nt)
        def _():
            wdc = wd_ref[...].reshape(CH, D)
            for s in range(TM // SUB):
                r = pl.ds(pl.multiple_of(t * TM + s * SUB, SUB), SUB)
                rr = slice(s * SUB, (s + 1) * SUB)
                g = jnp.concatenate([x[rr, :] for x in gs], axis=1)
                u = jnp.concatenate([x[rr, :] for x in us], axis=1)
                dh = dot_nt(dy_v[r, :], wdc).astype(bf16).astype(f32)
                sig = sigmoid(g)
                silu = g * sig
                dg_s[r, :] = (dh * u * (sig + silu - silu * sig)).astype(bf16)
                du_s[r, :] = (dh * silu).astype(bf16)
                hid_s[r, :] = (silu * u).astype(bf16)

        products(t, nt, a_v, dy_v, dg_s, du_s, hid_s, tmpg, tmpu, tmpd, send_ref, keep_ref)

    col = [pl.BlockSpec((TM, 128), functools.partial(lambda q, t: (jnp.minimum(t, nt - 1), q * NC + j), q)) for q in range(4)]
    return pl.pallas_call(
        body,
        grid=(nt + 3,),
        in_specs=[pl.BlockSpec(memory_space=pl.ANY)] * 2
        + col
        + col
        + [pl.BlockSpec((4, 128, D), lambda t: (0, j, 0), pipeline_mode=pl.Buffered(1))],
        out_specs=GRAD_SPECS,
        out_shape=GRADS,
        scratch_shapes=PRODUCT_SCRATCH + [pltpu.SemaphoreType.DMA((2, nt))],
        compiler_params=PARAMS,
        cost_estimate=cost(4, CH, 30_000_000),
        name=f"backward_bottom_{j}",
    )(a, dy, *[gate] * 4, *[up] * 4, wd.reshape(4, 640, D))


def summed(send, keep):
    wide = lambda v: v.astype(f32)
    got = lax.ppermute(send, "s", [(i, i ^ 1) for i in range(4)])
    theirs = (wide(keep[0]) + wide(got[0])).astype(bf16)
    other = lax.ppermute(theirs, "s", [(i, i ^ 2) for i in range(4)])
    ours = (wide(keep[1]) + wide(got[1]) + wide(other)).astype(bf16)
    copy = lax.ppermute(ours, "r", [(0, 1), (1, 0)])
    return (wide(ours) + wide(copy)).astype(bf16)


def blocks(chunks):
    g = jnp.stack(chunks)
    two = [g[:, 256 * i : 256 * i + 256].reshape(NC, 256, 4, 128).transpose(1, 2, 0, 3).reshape(256, FF) for i in range(2)]
    return two + [g[:, 512:].reshape(NC, 2, 128, CH).transpose(0, 2, 1, 3).reshape(640, D)]


def adamw(w, m, v, g):
    m = 0.9 * m + 0.1 * g
    v = 0.95 * v + 0.05 * g * g
    step = m * lax.rsqrt(v + 1e-8) + 0.1 * w
    return (w - 0.02 * step).astype(bf16), m, v


def solution(mesh):
    def step(x, dy, *arrays):
        weights, m, v = (arrays[i : i + 3] for i in (0, 3, 6))
        x, dy = x[0], dy[0]
        full = [[lax.all_gather(w[n], "s", axis=0, tiled=True) for w in weights] for n in range(2)]
        a0, gate, up, hid = forward_up(x, full[0][0], full[0][1])
        h, a1 = forward_down(x, hid, full[0][2])
        top = [backward_top(j, a1, dy, *full[1]) for j in range(NC)]
        g1 = [summed(send, keep) for _, _, send, keep in top]
        dh = backward_through([c[0] for c in top], [c[1] for c in top], full[1][0], full[1][1], h, dy)
        g0 = [summed(*backward_bottom(j, a0, dh, gate, up, full[0][2])) for j in range(NC)]
        mine = [blocks(g0), blocks(g1)]
        gradients = [jnp.stack([mine[n][i] for n in range(2)]).astype(f32) for i in range(3)]
        squares = lax.psum(sum(jnp.sum(g * g) for g in gradients), "s")
        count = lax.psum(1, "s") * sum(g.size for g in gradients)
        factor = jnp.minimum(1.0, 0.5 * lax.rsqrt(squares / count + 1e-30))
        new = [adamw(w.astype(f32), m, v, g * factor) for w, m, v, g in zip(weights, m, v, gradients, strict=True)]
        return tuple(one[which] for which in range(3) for one in new)

    states, cut = P(("rep", "r", "s"), None, None), P(None, "s", None)
    return jax.shard_map(
        step,
        mesh=mesh,
        in_specs=(states, states) + (cut,) * 9,
        out_specs=(P("rep", "s", None),) * 9,
        check_vma=False,
    )
```

```python
import jax
import jax.numpy as jnp
from jax import lax
from jax.experimental import pallas as pl
from jax.experimental.pallas import tpu as pltpu
from jax.sharding import PartitionSpec as P

TOK, D, FF = 4096, 1024, 2560
NC, CH = 5, 512
TM, SUB = 512, 256
NT = TOK // TM
bf16, f32 = jnp.bfloat16, jnp.float32
MESH = pl.DeviceIdType.MESH
ANY = pl.BlockSpec(memory_space=pl.ANY)
VMEM, DMA = pltpu.VMEM, pltpu.SemaphoreType.DMA


def sds(shape, dtype=bf16):
    return jax.ShapeDtypeStruct(shape, dtype)


def params(collective_id=None):
    return pltpu.CompilerParams(vmem_limit_bytes=63 * 1024 * 1024, collective_id=collective_id, has_side_effects=collective_id is not None)


def dot(a, b):
    return jnp.dot(a, b, preferred_element_type=f32)


def dot_nt(a, b):
    return lax.dot_general(a, b, (((1,), (1,)), ((), ())), preferred_element_type=f32)


def dot_tn(a, b):
    return lax.dot_general(a, b, (((0,), (0,)), ((), ())), preferred_element_type=f32)


def cost(products, width, nbytes):
    return pl.CostEstimate(flops=products * 2 * TOK * D * width, bytes_accessed=nbytes, transcendentals=0)


def scale_of(wide):
    return lax.rsqrt(jnp.mean(wide * wide, -1, keepdims=True) + 1e-6)


def sigmoid(g):
    return 0.5 * jnp.tanh(0.5 * g) + 0.5


def places():
    s, r = lax.axis_index("s"), lax.axis_index("r")
    xx, core = s // 2, s % 2
    return s, xx, core, r, {"s": s + 1 - 2 * core}, {"s": s + 2 - 4 * xx}, {"r": 1 - r}


def meet(*others):
    barrier = pltpu.get_barrier_semaphore()
    for other in others:
        pl.semaphore_signal(barrier, inc=1, device_id=other, device_id_type=MESH)
    pl.semaphore_wait(barrier, len(others))


def remote(src, dst, send, recv, other):
    return pltpu.make_async_remote_copy(src_ref=src, dst_ref=dst, send_sem=send, recv_sem=recv, device_id=other, device_id_type=MESH)


UNITS = 14


def forward(x, wg, wu, wd):
    def body(x_ref, wg_ref, wu_ref, wd_ref, xt_ref, wd0, wg1, wu1, wd1, a0_ref, g_ref, u_ref, h_ref, a1_ref, a_v, wg0, wu0, wd_v, hid_v, st_w, st_d, send, recv, local):
        i = pl.program_id(0)
        s, xx, core, r, mate, along_x, along_y = places()
        far, diag = s + 2 - 4 * xx, s + 1 - 2 * core + 2 - 4 * xx
        full = (wg0, wu0) * NC + (wd0, wg1, wu1, wd1)
        mine = (wg_ref.at[0], wu_ref.at[0]) * NC + (wd_ref.at[0], wg_ref.at[1], wu_ref.at[1], wd_ref.at[1])

        def part(ref, k, first, rows):
            first = pl.multiple_of(first, 64)
            if k < 2 * NC:
                return ref.at[pl.ds(first, rows), pl.ds(k // 2 * CH, CH)]
            return ref.at[pl.ds(first, rows)]

        def place(k, owner, half=None):
            rows = 640 if k in (10, 13) else 256
            if half is None:
                return part(full[k], k, owner * rows, rows)
            return part(full[k], k, owner * rows + half * (rows // 2), rows // 2)

        def own(k, half=None):
            rows = 640 if k in (10, 13) else 256
            return part(mine[k], k, 0, rows) if half is None else part(mine[k], k, half * (rows // 2), rows // 2)

        def to_mate(k):
            return remote(own(k), place(k, s), send.at[0, k], recv.at[0, k], mate)

        def to_x(k):
            return remote(own(k, r), place(k, s, r), send.at[1, k], recv.at[1, k], along_x)

        def to_y(k):
            return remote(place(k, far, r), place(k, far, r), send.at[2, k], recv.at[2, k], along_y)

        def x_to_mate(k):
            return remote(place(k, far, r), place(k, far, r), send.at[3, k], recv.at[3, k], mate)

        def y_to_mate(k):
            return remote(place(k, far, 1 - r), place(k, far, 1 - r), send.at[4, k], recv.at[4, k], mate)

        def got(kind, k):
            where = ((s + 1 - 2 * core, None), (far, r), (far, 1 - r), (diag, r), (diag, 1 - r))[kind]
            here = place(k, *where)
            remote(here, here, send.at[kind, k], recv.at[kind, k], mate).wait_recv()

        def pass_x(k):
            got(1, k)
            to_y(k).start()
            x_to_mate(k).start()

        def pass_y(k):
            got(2, k)
            y_to_mate(k).start()

        def complete(k):
            for kind in (0, 3, 4):
                got(kind, k)

        x_in = lambda t: pltpu.make_async_copy(x_ref.at[pl.ds(t * TM, TM)], a_v.at[pl.ds(t * TM, TM)], local.at[t])
        a_out = pltpu.make_async_copy(a_v, a0_ref, local.at[8])
        own_in = [pltpu.make_async_copy(m, f.at[pl.ds(pl.multiple_of(s * 256, 256), 256)], local.at[9 + n]) for n, (m, f) in enumerate(((mine[0], wg0), (mine[1], wu0)))]
        stage = []
        for n, k in enumerate((10, 11, 13, 12)):
            buf = st_d if k in (10, 13) else st_w
            stage.append((pltpu.make_async_copy(own(k), buf, local.at[11 + n]), pltpu.make_async_copy(buf, place(k, s), local.at[15 + n])))
        wd_in = pltpu.make_async_copy(wd0, wd_v, local.at[19])

        @pl.when(i == 0)
        def _():
            for t in range(NT):
                x_in(t).start()
            meet(mate, along_x, along_y)
            for k in range(2 * NC):
                to_x(k).start()
                to_mate(k).start()
            for k in range(2 * NC, UNITS):
                to_x(k).start()
            for c in own_in:
                c.start()
            for c, _ in stage[:2]:
                c.start()

            def norm(t, _):
                x_in(t).wait()
                for n in range(TM // SUB):
                    rows = pl.ds(pl.multiple_of(t * TM + n * SUB, SUB), SUB)
                    wide = a_v[rows, :].astype(f32)
                    a_v[rows, :] = (wide * scale_of(wide)).astype(bf16)
                return 0

            pass_x(0)
            pass_x(1)
            lax.fori_loop(0, NT, norm, 0)
            a_out.start()
            for k in range(2 * NC, UNITS):
                to_mate(k).start()
            for c, d in stage[:2]:
                c.wait()
                d.start()
            for k in (2, 3):
                pass_x(k)
            for k in (0, 1):
                pass_y(k)
            for c in own_in:
                c.wait()

        for c in range(NC):

            @pl.when(i == c * NT)
            def _(c=c):
                complete(2 * c)
                complete(2 * c + 1)

            if c + 1 < NC:

                @pl.when(i == c * NT + 4)
                def _(c=c):
                    if c + 2 < NC:
                        pass_x(2 * c + 4)
                        pass_x(2 * c + 5)
                    pass_y(2 * c + 2)
                    pass_y(2 * c + 3)

        @pl.when(i == 10)
        def _():
            for (_, d), (c, _) in zip(stage[:2], stage[2:]):
                d.wait()
                c.start()

        @pl.when(i == 18)
        def _():
            for c, d in stage[2:]:
                c.wait()
                d.start()

        for at, do, k in ((25, pass_x, 10), (37, pass_y, 10), (36, pass_x, 11), (43, pass_x, 12), (44, pass_y, 11)):

            @pl.when(i == at)
            def _(do=do, k=k):
                do(k)

        for c in range(NC):

            @pl.when(i // NT == c)
            def _(c=c):
                cols = slice(c * CH, (c + 1) * CH)
                for n in range(TM // SUB):
                    rows = pl.ds(pl.multiple_of(i % NT * TM + n * SUB, SUB), SUB)
                    a = a_v[rows, :]
                    g, u = dot(a, wg0[:, cols]), dot(a, wu0[:, cols])
                    g_ref[n * SUB : (n + 1) * SUB, :] = g
                    u_ref[n * SUB : (n + 1) * SUB, :] = u
                    hid_v[rows, cols] = (g * sigmoid(g) * u).astype(bf16)

        @pl.when(i == NC * NT)
        def _():
            complete(10)
            wd_in.start()
            wd_in.wait()

        @pl.when(i >= NC * NT)
        def _():
            rows = pl.ds(pl.multiple_of(i % NT * TM, TM), TM)
            y = dot(hid_v[rows, :], wd_v[...]).astype(bf16)
            h = (xt_ref[...].astype(f32) + y.astype(f32)).astype(bf16)
            h_ref[...] = h
            wide = h.astype(f32)
            a1_ref[...] = (wide * scale_of(wide)).astype(bf16)

        @pl.when(i == NC * NT + NT - 1)
        def _():
            pass_x(13)
            pass_y(12)
            pass_y(13)
            for k in (11, 12, 13):
                complete(k)
            for k in range(UNITS):
                for copy in (to_mate, to_x, to_y, x_to_mate, y_to_mate):
                    copy(k).wait_send()
            for _, d in stage[2:]:
                d.wait()
            a_out.wait()

    late = lambda i: (jnp.maximum(i - NC * NT, 0), 0)
    tile = lambda i: (jnp.where(i < NC * NT, i % NT, NT - 1), jnp.minimum(i // NT, NC - 1))
    return pl.pallas_call(
        body,
        grid=(NC * NT + NT,),
        in_specs=[ANY] * 4 + [pl.BlockSpec((TM, D), late)],
        out_specs=[ANY] * 5 + [pl.BlockSpec((TM, CH), tile)] * 2 + [pl.BlockSpec((TM, D), late)] * 2,
        out_shape=[sds((FF, D)), sds((D, FF)), sds((D, FF)), sds((FF, D)), sds((TOK, D)), sds((TOK, FF), f32), sds((TOK, FF), f32), sds((TOK, D)), sds((TOK, D))],
        scratch_shapes=[
            VMEM((TOK, D), bf16),
            VMEM((D, FF), bf16),
            VMEM((D, FF), bf16),
            VMEM((FF, D), bf16),
            VMEM((TOK, FF), bf16),
            VMEM((256, FF), bf16),
            VMEM((640, D), bf16),
            DMA((5, UNITS)),
            DMA((5, UNITS)),
            DMA((20,)),
        ],
        compiler_params=params(0),
        cost_estimate=cost(3, FF, 150_000_000),
        name="forward",
    )(x, wg, wu, wd, x)


class Summing:
    SHAPES = [
        VMEM((3, 2, 2, 256, CH), bf16),
        VMEM((2, 3, 2, 256, CH), bf16),
        VMEM((2, 3, 256, CH), bf16),
        VMEM((2, 3, 256, CH), bf16),
        VMEM((3, 256, CH), bf16),
        VMEM((3, 256, CH), bf16),
        VMEM((8, CH), f32),
        DMA((3, 2, 3)),
        DMA((3, 2, 3)),
        DMA((3, 4)),
    ]

    def __init__(self, refs, outs):
        self.sk, self.r1, self.r2, self.r3, self.ours, self.fin, self.squares, self.send, self.recv, self.local = refs
        self.outs = outs
        _, self.xx, self.core, _, self.mate, self.along_x, self.along_y = places()

    def meet(self):
        meet(self.mate, self.along_x, self.along_y)
        self.squares[...] = jnp.zeros_like(self.squares)

    def put(self, p, value):
        value = value.astype(bf16)
        for o in range(4):
            kx = self.xx if o // 2 else 1 - self.xx
            kc = self.core if o % 2 else 1 - self.core
            if p < 2:
                self.sk[p, kc, kx] = value[256 * o : 256 * o + 256]
            else:
                self.sk[p, kc, kx, 0:128] = value[128 * o : 128 * o + 128, 0:CH]
                self.sk[p, kc, kx, 128:256] = value[128 * o : 128 * o + 128, CH : 2 * CH]

    def copy(self, stage, j, p):
        b = j % 2
        src, dst, to = (
            (self.sk.at[p, 0], self.r1.at[b, p], self.mate),
            (self.sk.at[p, 1, 0], self.r2.at[b, p], self.along_x),
            (self.ours.at[p], self.r3.at[b, p], self.along_y),
        )[stage]
        return remote(src, dst, self.send.at[stage, b, p], self.recv.at[stage, b, p], to)

    def start(self, j, p):
        self.copy(0, j, p).start()

    def over_x(self, j, p):
        self.copy(0, j, p).wait()
        self.sk[p, 1, 0] = (self.sk[p, 1, 0].astype(f32) + self.r1[j % 2, p, 0].astype(f32)).astype(bf16)
        self.copy(1, j, p).start()

    def over_y(self, j, p):
        self.copy(1, j, p).wait()
        b = j % 2
        self.ours[p] = (self.sk[p, 1, 1].astype(f32) + self.r1[b, p, 1].astype(f32) + self.r2[b, p].astype(f32)).astype(bf16)
        self.copy(2, j, p).start()

    def out(self, j, p):
        if p < 2:
            return [
                pltpu.make_async_copy(
                    self.fin.at[p, :, pl.ds(128 * q, 128)], self.outs[p].at[:, pl.ds(pl.multiple_of(640 * q + 128 * j, 128), 128)], self.local.at[p, q]
                )
                for q in range(4)
            ]
        rows = pl.ds(pl.multiple_of(128 * j, 128), 128)
        return [pltpu.make_async_copy(self.fin.at[p, pl.ds(128 * q, 128)], self.outs[p].at[rows, pl.ds(CH * q, CH)], self.local.at[p, q]) for q in range(2)]

    def finish(self, j, p):
        self.copy(2, j, p).wait()
        g = (self.ours[p].astype(f32) + self.r3[j % 2, p].astype(f32)).astype(bf16)
        self.fin[p] = g
        g = g.astype(f32)
        self.squares[...] += jnp.sum((g * g).reshape(32, 8, CH), axis=0)
        for c in self.out(j, p):
            c.start()

    def flushed(self, j, p):
        for c in self.out(j, p):
            c.wait()

    def beside(self, j, t, steps):
        for at, what in (
            (1, lambda: (self.over_y(j - 1, 0), self.over_x(j - 1, 2))),
            (7, lambda: self.over_y(j - 1, 1)),
            (8, lambda: self.finish(j - 1, 0)),
            (9, lambda: (self.over_y(j - 1, 2), self.finish(j - 1, 1))),
            (10, lambda: (self.flushed(j - 1, 0), self.flushed(j - 1, 1))),
        ):
            if at in steps:

                @pl.when((j >= 1) & (t == at))
                def _(what=what):
                    what()

        if 4 in steps:

            @pl.when((j >= 2) & (t == 4))
            def _():
                self.finish(j - 2, 2)

            @pl.when((j >= 2) & (t == 6))
            def _():
                self.flushed(j - 2, 2)


def products(j, t, last, a_v, dy_v, dg_s, du_s, hid_s, sums):
    sums.beside(j, t, range(NT))

    @pl.when(t == NT)
    def _():
        value = dot_tn(a_v[...], dg_s[...])
        sums.beside(j, t, [NT])
        sums.put(0, value)

        @pl.when(j <= last)
        def _():
            sums.start(j, 0)

    @pl.when(t == NT + 1)
    def _():
        value = dot_tn(a_v[...], du_s[...])
        sums.beside(j, t, [NT + 1])
        sums.put(1, value)

        @pl.when(j <= last)
        def _():
            sums.over_x(j, 0)
            sums.start(j, 1)

    @pl.when(t == NT + 2)
    def _():
        value = dot_tn(hid_s[...], dy_v[...])
        sums.beside(j, t, [NT + 2])
        sums.put(2, value)

        @pl.when(j <= last)
        def _():
            sums.over_x(j, 1)
            sums.start(j, 2)


def load_tiles(j, t, pairs, sems):
    rows = lambda i: pl.ds(pl.multiple_of(i * TM, TM), TM)
    copies = lambda i: [pltpu.make_async_copy(src.at[rows(i)], dst.at[rows(i)], sems.at[n, i]) for n, (src, dst) in enumerate(pairs)]

    @pl.when((j == 0) & (t == 0))
    def _():
        for i in range(NT):
            for c in copies(i):
                c.start()

    @pl.when((j == 0) & (t < NT))
    def _():
        for c in copies(t):
            c.wait()


BACKWARD = [VMEM((TOK, D), bf16)] * 2 + [VMEM((TOK, CH), bf16)] * 3 + [DMA((2, NT))]
BLOCKS = [sds((256, FF)), sds((256, FF)), sds((640, D))]
SQUARES = sds((8, CH), f32)
SQUARES_SPEC = pl.BlockSpec((8, CH), lambda *_: (0, 0))


def backward_top(a, dy, wg, wu, wd):
    def body(a_ref, dy_ref, *rest):
        wgs, wus, wd_ref = rest[0:4], rest[4:8], rest[8]
        dg_ref, du_ref, og, ou, od, sk_ref, sq_ref, a_v, dy_v, dg_s, du_s, hid_s, sems, wgc, wuc, last_sem, *comm = rest[9:]
        j, t = pl.program_id(0), pl.program_id(1)
        sums = Summing(comm, (og, ou, od))
        load_tiles(j, t, ((a_ref, a_v), (dy_ref, dy_v)), sems)

        @pl.when((j == 0) & (t == 0))
        def _():
            sums.meet()

        @pl.when(t == 0)
        def _():
            wgc[...] = jnp.concatenate([w[...] for w in wgs], axis=1)
            wuc[...] = jnp.concatenate([w[...] for w in wus], axis=1)

        @pl.when(t < NT)
        def _():
            wdc = wd_ref[...].reshape(CH, D)
            for n in range(TM // SUB):
                r = pl.ds(pl.multiple_of(t * TM + n * SUB, SUB), SUB)
                x = a_v[r, :]
                g, u = dot(x, wgc[...]), dot(x, wuc[...])
                dh = dot_nt(dy_v[r, :], wdc).astype(bf16).astype(f32)
                sig = sigmoid(g)
                silu = g * sig
                dg = (dh * u * (sig + silu - silu * sig)).astype(bf16)
                du = (dh * silu).astype(bf16)
                hid_s[r, :] = (silu * u).astype(bf16)
                dg_s[r, :] = dg
                du_s[r, :] = du
                dg_ref[n * SUB : (n + 1) * SUB, :] = dg
                du_ref[n * SUB : (n + 1) * SUB, :] = du

        products(j, t, NC - 2, a_v, dy_v, dg_s, du_s, hid_s, sums)

        @pl.when((j == NC - 1) & (t == NT + 2))
        def _():
            give = pltpu.make_async_copy(sums.sk, sk_ref, last_sem)
            give.start()
            sums.finish(NC - 2, 2)
            sums.flushed(NC - 2, 2)
            sq_ref[...] = sums.squares[...]
            give.wait()

    col = [pl.BlockSpec((D, 128), lambda j, t, q=q: (0, q * NC + j)) for q in range(4)]
    tile = pl.BlockSpec((TM, CH), lambda j, t: (jnp.minimum(t, NT - 1), j))
    return pl.pallas_call(
        body,
        grid=(NC, NT + 3),
        in_specs=[ANY] * 2 + col + col + [pl.BlockSpec((4, 128, D), lambda j, t: (0, j, 0))],
        out_specs=[tile, tile] + [ANY] * 4 + [SQUARES_SPEC],
        out_shape=[sds((TOK, FF))] * 2 + BLOCKS + [sds((3, 2, 2, 256, CH)), SQUARES],
        scratch_shapes=BACKWARD + [VMEM((D, CH), bf16)] * 2 + [DMA] + Summing.SHAPES,
        compiler_params=params(1),
        cost_estimate=cost(6, FF, 80_000_000),
        name="backward_top",
    )(a, dy, *[wg] * 4, *[wu] * 4, wd.reshape(4, 640, D))


def backward_through(dg, du, wg, wu, h, dy, sk, og, ou, od):
    TB = 256
    steps = TOK // TB

    def body(dg_ref, du_ref, wg_ref, wu_ref, h_ref, dy_ref, sk_ref, _a, _b, _c, out_ref, og, ou, od, sq_ref, sem, *comm):
        t = pl.program_id(0)
        sums = Summing(comm, (og, ou, od))

        @pl.when(t == 0)
        def _():
            take = pltpu.make_async_copy(sk_ref, sums.sk, sem)
            take.start()
            sums.meet()
            take.wait()
            for p in range(3):
                sums.start(NC - 1, p)

        natural = lambda ref: jnp.concatenate([ref[:, CH * j + 128 * q : CH * j + 128 * q + 128] for q in range(4) for j in range(NC)], axis=1)
        da = dot_nt(natural(dg_ref), wg_ref[...]).astype(bf16).astype(f32) + dot_nt(natural(du_ref), wu_ref[...]).astype(bf16).astype(f32)
        da = da.astype(bf16).astype(f32)
        wide = h_ref[...].astype(f32)
        scale = scale_of(wide)
        along = jnp.sum(da * wide, -1, keepdims=True) * (scale * scale * scale * (1.0 / D))
        dh = (da * scale - wide * along).astype(bf16)
        out_ref[...] = (dy_ref[...].astype(f32) + dh.astype(f32)).astype(bf16)

        for p in range(3):
            for at, what in ((1 + p, sums.over_x), (5 + 2 * p, sums.over_y), (9 + 2 * p, sums.finish), (15, sums.flushed)):

                @pl.when(t == at)
                def _(what=what, p=p):
                    what(NC - 1, p)

        @pl.when(t == steps - 1)
        def _():
            sq_ref[...] = sums.squares[...]

    row = lambda n: pl.BlockSpec((TB, n), lambda t: (t, 0))
    once = pl.BlockSpec((D, FF), lambda t: (0, 0), pipeline_mode=pl.Buffered(1))
    return pl.pallas_call(
        body,
        grid=(steps,),
        in_specs=[row(FF)] * 2 + [once] * 2 + [row(D)] * 2 + [ANY] * 4,
        out_specs=[row(D)] + [ANY] * 3 + [SQUARES_SPEC],
        out_shape=[sds((TOK, D))] + BLOCKS + [SQUARES],
        input_output_aliases={7: 1, 8: 2, 9: 3},
        scratch_shapes=[DMA] + Summing.SHAPES,
        compiler_params=params(2),
        cost_estimate=cost(2, FF, 80_000_000),
        name="backward_through",
    )(dg, du, wg, wu, h, dy, sk, og, ou, od)


def backward_bottom(a, dy, gate, up, wd):
    def body(a_ref, dy_ref, *rest):
        gs, us, wd_ref = rest[0:4], rest[4:8], rest[8]
        og, ou, od, sq_ref, a_v, dy_v, dg_s, du_s, hid_s, sems, *comm = rest[9:]
        j, t = pl.program_id(0), pl.program_id(1)
        sums = Summing(comm, (og, ou, od))
        load_tiles(j, t, ((a_ref, a_v), (dy_ref, dy_v)), sems)

        @pl.when((j == 0) & (t == 0))
        def _():
            sums.meet()

        @pl.when(t < NT)
        def _():
            wdc = wd_ref[...].reshape(CH, D)
            for n in range(TM // SUB):
                r = pl.ds(pl.multiple_of(t * TM + n * SUB, SUB), SUB)
                rr = slice(n * SUB, (n + 1) * SUB)
                g = jnp.concatenate([v[rr, :] for v in gs], axis=1)
                u = jnp.concatenate([v[rr, :] for v in us], axis=1)
                dh = dot_nt(dy_v[r, :], wdc).astype(bf16).astype(f32)
                sig = sigmoid(g)
                silu = g * sig
                dg_s[r, :] = (dh * u * (sig + silu - silu * sig)).astype(bf16)
                du_s[r, :] = (dh * silu).astype(bf16)
                hid_s[r, :] = (silu * u).astype(bf16)

        products(j, t, NC - 1, a_v, dy_v, dg_s, du_s, hid_s, sums)

        @pl.when((j == NC - 1) & (t == NT + 2))
        def _():
            e = NC - 1
            sums.finish(e - 1, 2)
            sums.over_y(e, 0)
            sums.over_x(e, 2)
            sums.over_y(e, 1)
            sums.finish(e, 0)
            sums.flushed(e - 1, 2)
            sums.over_y(e, 2)
            for p in (1, 2):
                sums.finish(e, p)
            for p in range(3):
                sums.flushed(e, p)
            sq_ref[...] = sums.squares[...]

    col = [pl.BlockSpec((TM, 128), lambda j, t, q=q: (jnp.minimum(t, NT - 1), q * NC + j)) for q in range(4)]
    return pl.pallas_call(
        body,
        grid=(NC, NT + 3),
        in_specs=[ANY] * 2 + col + col + [pl.BlockSpec((4, 128, D), lambda j, t: (0, j, 0))],
        out_specs=[ANY] * 3 + [SQUARES_SPEC],
        out_shape=BLOCKS + [SQUARES],
        scratch_shapes=BACKWARD + Summing.SHAPES,
        compiler_params=params(3),
        cost_estimate=cost(4, FF, 120_000_000),
        name="backward_bottom",
    )(a, dy, *[gate] * 4, *[up] * 4, wd.reshape(4, 640, D))


def adamw(factor, weights, m, v, g0, g1):
    parts = 4

    def body(factor_ref, *refs):
        w, m, v, g0, g1, nw, nm, nv = (refs[3 * n : 3 * n + 3] for n in range(8))
        factor = factor_ref[0]

        def update(g, k):
            g = g[...].astype(f32) * factor
            new_m = 0.9 * m[k][0] + 0.1 * g
            new_v = 0.95 * v[k][0] + 0.05 * g * g
            move = new_m * lax.rsqrt(new_v + 1e-8) + 0.1 * w[k][0].astype(f32)
            nm[k][0] = new_m
            nv[k][0] = new_v
            nw[k][0] = (w[k][0].astype(f32) - 0.02 * move).astype(bf16)

        for n, g in enumerate((g0, g1)):

            @pl.when(pl.program_id(0) == n)
            def _(g=g):
                for k in range(3):
                    update(g[k], k)

    shapes = [(256 // parts, FF)] * 2 + [(640 // parts, D)]
    whole = [pl.BlockSpec((1, *s), lambda n, t: (n, t, 0)) for s in shapes]
    low = [pl.BlockSpec(s, lambda n, t: (jnp.where(n == 0, t, parts - 1), 0)) for s in shapes]
    high = [pl.BlockSpec(s, lambda n, t: (jnp.where(n == 1, t, 0), 0)) for s in shapes]
    return pl.pallas_call(
        body,
        grid=(2, parts),
        in_specs=[pl.BlockSpec(memory_space=pltpu.SMEM)] + whole * 3 + low + high,
        out_specs=whole * 3,
        out_shape=[sds(w.shape, d) for d in (bf16, f32, f32) for w in weights],
        compiler_params=params(),
        name="adamw",
    )(factor, *weights, *m, *v, *g0, *g1)


def solution(mesh):
    def step(x, dy, *arrays):
        weights, m, v = (arrays[i : i + 3] for i in (0, 3, 6))
        x, dy = x[0], dy[0]
        wd0, wg1, wu1, wd1, a0, gate, up, h, a1 = forward(x, *weights)
        dg, du, *g1, sk, sq1 = backward_top(a1, dy, wg1, wu1, wd1)
        dh, *g1, sq2 = backward_through(dg, du, wg1, wu1, h, dy, sk, *g1)
        *g0, sq3 = backward_bottom(a0, dh, gate, up, wd0)
        squares = lax.psum(jnp.sum(sq1 + sq2 + sq3), "s")
        count = lax.psum(1, "s") * sum(w.size for w in weights)
        factor = jnp.minimum(1.0, 0.5 * lax.rsqrt(squares / count + 1e-30))
        return tuple(adamw(factor.reshape(1), weights, m, v, g0, g1))

    states, cut = P(("rep", "r", "s"), None, None), P(None, "s", None)
    return jax.shard_map(
        step,
        mesh=mesh,
        in_specs=(states, states) + (cut,) * 9,
        out_specs=(P("rep", "s", None),) * 9,
        check_vma=False,
    )
```

```python
import jax
import jax.numpy as jnp
from jax import lax
from jax.experimental import pallas as pl
from jax.experimental.pallas import tpu as pltpu
from jax.sharding import PartitionSpec as P

TOK, D, FF = 4096, 1024, 2560
NC, CH = 5, 512
TM, SUB = 1024, 256
NT = TOK // TM
FM, FT = 512, 8
bf16, f32 = jnp.bfloat16, jnp.float32
MESH = pl.DeviceIdType.MESH
ANY = pl.BlockSpec(memory_space=pl.ANY)
VMEM, DMA = pltpu.VMEM, pltpu.SemaphoreType.DMA


def sds(shape, dtype=bf16):
    return jax.ShapeDtypeStruct(shape, dtype)


def params(collective_id=None):
    return pltpu.CompilerParams(vmem_limit_bytes=63 * 1024 * 1024, collective_id=collective_id, has_side_effects=collective_id is not None)


def dot(a, b):
    return jnp.dot(a, b, preferred_element_type=f32)


def dot_nt(a, b):
    return lax.dot_general(a, b, (((1,), (1,)), ((), ())), preferred_element_type=f32)


def dot_tn(a, b):
    return lax.dot_general(a, b, (((0,), (0,)), ((), ())), preferred_element_type=f32)


def cost(products, width, nbytes):
    return pl.CostEstimate(flops=products * 2 * TOK * D * width, bytes_accessed=nbytes, transcendentals=0)


def scale_of(wide):
    return lax.rsqrt(jnp.mean(wide * wide, -1, keepdims=True) + 1e-6)


def sigmoid(g):
    return 0.5 * jnp.tanh(0.5 * g) + 0.5


def places():
    s, r = lax.axis_index("s"), lax.axis_index("r")
    xx, core = s // 2, s % 2
    return s, xx, core, r, {"s": s + 1 - 2 * core}, {"s": s + 2 - 4 * xx}, {"r": 1 - r}


def meet(*others):
    barrier = pltpu.get_barrier_semaphore()
    for other in others:
        pl.semaphore_signal(barrier, inc=1, device_id=other, device_id_type=MESH)
    pl.semaphore_wait(barrier, len(others))


def remote(src, dst, send, recv, other):
    return pltpu.make_async_remote_copy(src_ref=src, dst_ref=dst, send_sem=send, recv_sem=recv, device_id=other, device_id_type=MESH)


UNITS = 14


class Routes:
    def __init__(self, place, mine, send, recv):
        self.place, self.mine, self.send, self.recv = place, mine, send, recv
        self.s, xx, core, self.r, self.mate, self.along_x, self.along_y = places()
        self.near = self.s + 1 - 2 * core
        self.far, self.diag = self.s + 2 - 4 * xx, self.near + 2 - 4 * xx

    def copy(self, kind, k):
        s, r, far = self.s, self.r, self.far
        src, dst, to = (
            lambda: (self.mine(k), self.place(k, s), self.mate),
            lambda: (self.mine(k, r), self.place(k, s, r), self.along_x),
            lambda: (self.place(k, far, r), self.place(k, far, r), self.along_y),
            lambda: (self.place(k, far, r), self.place(k, far, r), self.mate),
            lambda: (self.place(k, far, 1 - r), self.place(k, far, 1 - r), self.mate),
        )[kind]()
        return remote(src, dst, self.send.at[kind, k], self.recv.at[kind, k], to)

    def to_mate(self, k):
        self.copy(0, k).start()

    def to_x(self, k):
        self.copy(1, k).start()

    def got(self, kind, k):
        r = self.r
        here = self.place(k, *((self.near, None), (self.far, r), (self.far, 1 - r), (self.diag, r), (self.diag, 1 - r))[kind])
        remote(here, here, self.send.at[kind, k], self.recv.at[kind, k], self.mate).wait_recv()

    def pass_x(self, k):
        self.got(1, k)
        self.copy(2, k).start()
        self.copy(3, k).start()

    def pass_y(self, k):
        self.got(2, k)
        self.copy(4, k).start()

    def complete(self, k):
        for kind in (0, 3, 4):
            self.got(kind, k)

    def sent(self, k):
        for kind in range(5):
            self.copy(kind, k).wait_send()


def forward(x, wg, wu, wd):
    def body(x_ref, wg_ref, wu_ref, wd_ref, xt_ref, wd0, wg1, wu1, wd1, a0_ref, g_ref, u_ref, h_ref, a1_ref, a_v, wg0, wu0, wd_v, hid_v, st_g, st_u, st_d, st_c, send, recv, local):
        i = pl.program_id(0)
        s = lax.axis_index("s")
        full = (wg0, wu0) * NC + (wd0, wg1, wu1, wd1)
        blocks = (None,) * (2 * NC) + (wd_ref.at[0], wg_ref.at[1], wu_ref.at[1], wd_ref.at[1])

        def size(k):
            return 640 if k == 10 else 128 if k == 13 else 256

        def place(k, owner, half=None):
            rows = size(k)
            first, count = (0, rows) if half is None else (pl.multiple_of(half * (rows // 2), 64), rows // 2)
            if k == 13:
                return full[k].at[owner, pl.ds(first, count)]
            at = pl.ds(pl.multiple_of(owner * rows + first, 64), count)
            return full[k].at[k // 2, at] if k < 2 * NC else full[k].at[at]

        def mine(k, half=None):
            if k < 2 * NC:
                return place(k, s, half)
            rows = size(k)
            return blocks[k].at[pl.ds(0, rows) if half is None else pl.ds(pl.multiple_of(half * (rows // 2), 64), rows // 2)]

        routes = Routes(place, mine, send, recv)
        x_in = lambda t: pltpu.make_async_copy(x_ref.at[pl.ds(t * FM, FM)], a_v.at[pl.ds(t * FM, FM)], local.at[t])
        a_out = pltpu.make_async_copy(a_v, a0_ref, local.at[8])
        own_in = [pltpu.make_async_copy(m.at[0], st, local.at[9 + n]) for n, (m, st) in enumerate(((wg_ref, st_g), (wu_ref, st_u)))]
        stage = [
            (pltpu.make_async_copy(mine(k), buf, local.at[11 + n]), pltpu.make_async_copy(buf, place(k, s), local.at[15 + n]))
            for n, (k, buf) in enumerate(((10, st_d), (11, st_g), (12, st_u), (13, st_c)))
        ]
        wd_in = pltpu.make_async_copy(wd0, wd_v, local.at[19])

        @pl.when(i == 0)
        def _():
            for c in own_in:
                c.start()
            for t in range(FT):
                x_in(t).start()
            rows = pl.ds(pl.multiple_of(s * 256, 256), 256)
            for c, st, w in zip(own_in, (st_g, st_u), (wg0, wu0)):
                c.wait()
                for j in range(NC):
                    for q in range(4):
                        w[j, rows, 128 * q : 128 * q + 128] = st[:, 640 * q + 128 * j : 640 * q + 128 * j + 128]
            meet(routes.mate, routes.along_x, routes.along_y)
            for k in range(UNITS):
                routes.to_x(k)
            for k in range(2 * NC):
                routes.to_mate(k)
            for c, _ in stage:
                c.start()

            def norm(t, _):
                x_in(t).wait()
                for n in range(FM // SUB):
                    rows = pl.ds(pl.multiple_of(t * FM + n * SUB, SUB), SUB)
                    wide = a_v[rows, :].astype(f32)
                    a_v[rows, :] = (wide * scale_of(wide)).astype(bf16)
                return 0

            routes.pass_x(0)
            routes.pass_x(1)
            lax.fori_loop(0, FT, norm, 0)
            a_out.start()
            for k in range(2 * NC, UNITS):
                routes.to_mate(k)
            for c, d in stage:
                c.wait()
                d.start()
            for k in (2, 3):
                routes.pass_x(k)
            for k in (0, 1):
                routes.pass_y(k)

        for c in range(NC):

            @pl.when(i == c * FT)
            def _(c=c):
                routes.complete(2 * c)
                routes.complete(2 * c + 1)

        events = [(4, "y", 2), (4, "y", 3), (3, "x", 4), (3, "x", 5), (8, "x", 6), (8, "x", 7), (9, "y", 4), (9, "y", 5), (13, "x", 8), (13, "x", 9), (14, "y", 6), (14, "y", 7)]
        events += [(18, "y", 8), (18, "y", 9), (23, "x", 10), (32, "x", 11), (34, "y", 10), (41, "x", 12), (41, "y", 11), (42, "x", 13)]

        def event(which, k):
            (routes.pass_x if which == "x" else routes.pass_y)(k)

        for c in range(NC):

            @pl.when(i // FT == c)
            def _(c=c):
                for n in range(FM // SUB):
                    rows = pl.ds(pl.multiple_of(i % FT * FM + n * SUB, SUB), SUB)
                    a = a_v[rows, :]
                    g, u = dot(a, wg0[c]), dot(a, wu0[c])
                    g_ref[0, n * SUB : (n + 1) * SUB, :] = g
                    u_ref[0, n * SUB : (n + 1) * SUB, :] = u
                    hid = (g * sigmoid(g) * u).astype(bf16)
                    for q in range(4):
                        hid_v[rows, 640 * q + 128 * c : 640 * q + 128 * c + 128] = hid[:, 128 * q : 128 * q + 128]

        @pl.when(i == NC * FT)
        def _():
            routes.complete(10)
            stage[0][1].wait()
            wd_in.start()
            wd_in.wait()

        @pl.when(i >= NC * FT)
        def _():
            rows = pl.ds(pl.multiple_of(i % FT * FM, FM), FM)
            y = dot(hid_v[rows, :], wd_v[...]).astype(bf16)
            h = (xt_ref[...].astype(f32) + y.astype(f32)).astype(bf16)
            h_ref[...] = h
            wide = h.astype(f32)
            a1_ref[...] = (wide * scale_of(wide)).astype(bf16)

        for at in sorted({e[0] for e in events}):

            @pl.when(i == at)
            def _(at=at):
                for e in events:
                    if e[0] == at:
                        event(*e[1:])

        @pl.when(i == NC * FT + FT - 1)
        def _():
            routes.pass_y(12)
            routes.pass_y(13)
            for k in (11, 12, 13):
                routes.complete(k)
            for k in range(UNITS):
                routes.sent(k)
            for _, d in stage[1:]:
                d.wait()
            a_out.wait()

    late = lambda i: (jnp.maximum(i - NC * FT, 0), 0)
    tile = lambda i: (jnp.minimum(i // FT, NC - 1), jnp.where(i < NC * FT, i % FT, FT - 1), 0)
    return pl.pallas_call(
        body,
        grid=(NC * FT + FT,),
        in_specs=[ANY] * 4 + [pl.BlockSpec((FM, D), late)],
        out_specs=[ANY] * 5 + [pl.BlockSpec((1, FM, CH), tile)] * 2 + [pl.BlockSpec((FM, D), late)] * 2,
        out_shape=[sds((FF, D)), sds((D, FF)), sds((D, FF)), sds((4, 128, D)), sds((TOK, D)), sds((NC, TOK, CH), f32), sds((NC, TOK, CH), f32), sds((TOK, D)), sds((TOK, D))],
        scratch_shapes=[
            VMEM((TOK, D), bf16),
            VMEM((NC, D, CH), bf16),
            VMEM((NC, D, CH), bf16),
            VMEM((FF, D), bf16),
            VMEM((TOK, FF), bf16),
            VMEM((256, FF), bf16),
            VMEM((256, FF), bf16),
            VMEM((640, D), bf16),
            VMEM((128, D), bf16),
            DMA((5, UNITS)),
            DMA((5, UNITS)),
            DMA((20,)),
        ],
        compiler_params=params(0),
        cost_estimate=cost(3, FF, 150_000_000),
        name="forward",
    )(x, wg, wu, wd, x)


class Summing:
    SHAPES = [
        VMEM((3, 2, 2, 256, CH), bf16),
        VMEM((2, 3, 2, 256, CH), bf16),
        VMEM((2, 3, 256, CH), bf16),
        VMEM((2, 3, 256, CH), bf16),
        VMEM((3, 256, CH), bf16),
        VMEM((3, 256, CH), bf16),
        VMEM((256, CH), f32),
        DMA((3, 2, 3)),
        DMA((3, 2, 3)),
        DMA((3, 4)),
    ]

    def __init__(self, refs, outs):
        self.sk, self.r1, self.r2, self.r3, self.ours, self.fin, self.squares, self.send, self.recv, self.local = refs
        self.outs = outs
        _, self.xx, self.core, _, self.mate, self.along_x, self.along_y = places()

    def meet(self):
        meet(self.mate, self.along_x, self.along_y)
        self.squares[...] = jnp.zeros_like(self.squares)

    def where(self, o):
        return self.core if o % 2 else 1 - self.core, self.xx if o // 2 else 1 - self.xx

    def put(self, p, a, b):
        for n in range(4 if p < 2 else 2):
            value = dot_tn(a[:, 256 * n : 256 * n + 256], b[...]).astype(bf16)
            if p < 2:
                kc, kx = self.where(n)
                self.sk[p, kc, kx] = value
                continue
            for o in (0, 1):
                kc, kx = self.where(2 * n + o)
                for q in (0, 1):
                    self.sk[p, kc, kx, 128 * q : 128 * q + 128] = value[128 * o : 128 * o + 128, CH * q : CH * q + CH]

    def copy(self, stage, j, p):
        b = j % 2
        src, dst, to = (
            (self.sk.at[p, 0], self.r1.at[b, p], self.mate),
            (self.sk.at[p, 1, 0], self.r2.at[b, p], self.along_x),
            (self.ours.at[p], self.r3.at[b, p], self.along_y),
        )[stage]
        return remote(src, dst, self.send.at[stage, b, p], self.recv.at[stage, b, p], to)

    def start(self, j, p):
        self.copy(0, j, p).start()

    def over_x(self, j, p):
        self.copy(0, j, p).wait()
        self.sk[p, 1, 0] = (self.sk[p, 1, 0].astype(f32) + self.r1[j % 2, p, 0].astype(f32)).astype(bf16)
        self.copy(1, j, p).start()

    def over_y(self, j, p):
        self.copy(1, j, p).wait()
        b = j % 2
        self.ours[p] = (self.sk[p, 1, 1].astype(f32) + self.r1[b, p, 1].astype(f32) + self.r2[b, p].astype(f32)).astype(bf16)
        self.copy(2, j, p).start()

    def out(self, j, p):
        if p < 2:
            return [
                pltpu.make_async_copy(
                    self.fin.at[p, :, pl.ds(128 * q, 128)], self.outs[p].at[:, pl.ds(pl.multiple_of(640 * q + 128 * j, 128), 128)], self.local.at[p, q]
                )
                for q in range(4)
            ]
        rows = pl.ds(pl.multiple_of(128 * j, 128), 128)
        return [pltpu.make_async_copy(self.fin.at[p, pl.ds(128 * q, 128)], self.outs[p].at[rows, pl.ds(CH * q, CH)], self.local.at[p, q]) for q in range(2)]

    def finish(self, j, p):
        self.copy(2, j, p).wait()
        g = (self.ours[p].astype(f32) + self.r3[j % 2, p].astype(f32)).astype(bf16)
        self.fin[p] = g
        g = g.astype(f32)
        self.squares[...] += g * g
        for c in self.out(j, p):
            c.start()

    def total(self):
        return sum(self.squares[8 * n : 8 * n + 8, :] for n in range(32))

    def flushed(self, j, p):
        for c in self.out(j, p):
            c.wait()

    def beside(self, j, t, steps):
        for at, what in (
            (1, lambda: (self.over_y(j - 1, 0), self.over_x(j - 1, 2))),
            (NT, lambda: (self.over_y(j - 1, 1), self.finish(j - 1, 0))),
            (NT + 1, lambda: self.over_y(j - 1, 2)),
            (NT + 2, lambda: (self.finish(j - 1, 1), self.flushed(j - 1, 0), self.flushed(j - 1, 1))),
        ):
            if at in steps:

                @pl.when((j >= 1) & (t == at))
                def _(what=what):
                    what()

        if 2 in steps:

            @pl.when((j >= 2) & (t == 2))
            def _():
                self.finish(j - 2, 2)

            @pl.when((j >= 2) & (t == 3))
            def _():
                self.flushed(j - 2, 2)


def products(j, t, last, a_v, dy_v, dg_s, du_s, hid_s, sums):
    sums.beside(j, t, range(NT))

    @pl.when(t == NT)
    def _():
        sums.put(0, a_v, dg_s)
        sums.beside(j, t, [NT])

        @pl.when(j <= last)
        def _():
            sums.start(j, 0)

    @pl.when(t == NT + 1)
    def _():
        sums.put(1, a_v, du_s)
        sums.beside(j, t, [NT + 1])

        @pl.when(j <= last)
        def _():
            sums.over_x(j, 0)
            sums.start(j, 1)

    @pl.when(t == NT + 2)
    def _():
        sums.put(2, hid_s, dy_v)
        sums.beside(j, t, [NT + 2])

        @pl.when(j <= last)
        def _():
            sums.over_x(j, 1)
            sums.start(j, 2)


def load_tiles(j, t, pairs, sems):
    rows = lambda i: pl.ds(pl.multiple_of(i * TM, TM), TM)
    copies = lambda i: [pltpu.make_async_copy(src.at[rows(i)], dst.at[rows(i)], sems.at[n, i]) for n, (src, dst) in enumerate(pairs)]

    @pl.when((j == 0) & (t == 0))
    def _():
        for i in range(NT):
            for c in copies(i):
                c.start()

    @pl.when((j == 0) & (t < NT))
    def _():
        for c in copies(t):
            c.wait()


BACKWARD = [VMEM((TOK, D), bf16)] * 2 + [VMEM((TOK, CH), bf16)] * 3 + [DMA((2, NT))]
BLOCKS = [sds((256, FF)), sds((256, FF)), sds((640, D))]
SQUARES = sds((8, CH), f32)
SQUARES_SPEC = pl.BlockSpec((8, CH), lambda *_: (0, 0))


def backward_top(a, dy, wg, wu, wd_first, wd):
    def body(a_ref, dy_ref, *rest):
        wgs, wus, first_ref, wd_ref = rest[0:4], rest[4:8], rest[8], rest[9]
        dg_ref, du_ref, og, ou, od, sk_ref, sq_ref, a_v, dy_v, dg_s, du_s, hid_s, sems, wgc, wuc, last_sem, wd_v, send, recv, own_sem, *comm = rest[10:]
        j, t = pl.program_id(0), pl.program_id(1)
        sums = Summing(comm, (og, ou, od))
        load_tiles(j, t, ((a_ref, a_v), (dy_ref, dy_v)), sems)

        s = lax.axis_index("s")
        rows = lambda half: pl.ds(0, 128) if half is None else pl.ds(pl.multiple_of(64 * half, 64), 64)
        routes = Routes(
            lambda k, owner, half=None: wd_v.at[k, owner, rows(half)],
            lambda k, half=None: wd_v.at[k, s, rows(half)],
            send,
            recv,
        )
        own = [pltpu.make_async_copy(wd_ref.at[1, pl.ds(128 * k, 128)] if k else first_ref, wd_v.at[k, s] if k else wd_v.at[0], own_sem.at[k]) for k in range(NC)]
        later = range(1, NC)

        @pl.when((j == 0) & (t == 0))
        def _():
            for c in own:
                c.start()
            sums.meet()
            for c in own:
                c.wait()
            for k in later:
                routes.to_x(k)
            for k in later:
                routes.to_mate(k)

        @pl.when((j == 0) & (t == 3))
        def _():
            for k in later:
                routes.pass_x(k)

        @pl.when((j == 0) & (t == NT + 1))
        def _():
            for k in later:
                routes.pass_y(k)

        for k in later:

            @pl.when((j == k) & (t == 0))
            def _(k=k):
                routes.complete(k)

        @pl.when(t == 0)
        def _():
            wgc[...] = jnp.concatenate([w[...] for w in wgs], axis=1)
            wuc[...] = jnp.concatenate([w[...] for w in wus], axis=1)

        @pl.when(t < NT)
        def _():
            wdc = wd_v[j].reshape(CH, D)
            for n in range(TM // SUB):
                r = pl.ds(pl.multiple_of(t * TM + n * SUB, SUB), SUB)
                x = a_v[r, :]
                g, u = dot(x, wgc[...]), dot(x, wuc[...])
                dh = dot_nt(dy_v[r, :], wdc).astype(bf16).astype(f32)
                sig = sigmoid(g)
                silu = g * sig
                dg = (dh * u * (sig + silu - silu * sig)).astype(bf16)
                du = (dh * silu).astype(bf16)
                hid_s[r, :] = (silu * u).astype(bf16)
                dg_s[r, :] = dg
                du_s[r, :] = du
                dg_ref[n * SUB : (n + 1) * SUB, :] = dg
                du_ref[n * SUB : (n + 1) * SUB, :] = du

        products(j, t, NC - 2, a_v, dy_v, dg_s, du_s, hid_s, sums)

        @pl.when((j == NC - 1) & (t == NT + 2))
        def _():
            give = pltpu.make_async_copy(sums.sk, sk_ref, last_sem)
            give.start()
            sums.finish(NC - 2, 2)
            sums.flushed(NC - 2, 2)
            sq_ref[...] = sums.total()
            for k in later:
                routes.sent(k)
            give.wait()

    col = [pl.BlockSpec((D, 128), lambda j, t, q=q: (0, q * NC + j)) for q in range(4)]
    tile = pl.BlockSpec((TM, CH), lambda j, t: (jnp.minimum(t, NT - 1), j))
    return pl.pallas_call(
        body,
        grid=(NC, NT + 3),
        in_specs=[ANY] * 2 + col + col + [ANY] * 2,
        out_specs=[tile, tile] + [ANY] * 4 + [SQUARES_SPEC],
        out_shape=[sds((TOK, FF))] * 2 + BLOCKS + [sds((3, 2, 2, 256, CH)), SQUARES],
        scratch_shapes=BACKWARD + [VMEM((D, CH), bf16)] * 2 + [DMA, VMEM((NC, 4, 128, D), bf16), DMA((5, NC)), DMA((5, NC)), DMA((NC,))] + Summing.SHAPES,
        compiler_params=params(1),
        cost_estimate=cost(6, FF, 80_000_000),
        name="backward_top",
    )(a, dy, *[wg] * 4, *[wu] * 4, wd_first, wd)


def backward_through(dg, du, wg, wu, h, dy, sk, og, ou, od):
    TB = 256
    steps = TOK // TB

    def body(dg_ref, du_ref, wg_ref, wu_ref, h_ref, dy_ref, sk_ref, _a, _b, _c, out_ref, og, ou, od, sq_ref, sem, *comm):
        t = pl.program_id(0)
        sums = Summing(comm, (og, ou, od))

        @pl.when(t == 0)
        def _():
            take = pltpu.make_async_copy(sk_ref, sums.sk, sem)
            take.start()
            sums.meet()
            take.wait()
            for p in range(3):
                sums.start(NC - 1, p)

        natural = lambda ref: jnp.concatenate([ref[:, CH * j + 128 * q : CH * j + 128 * q + 128] for q in range(4) for j in range(NC)], axis=1)
        da = dot_nt(natural(dg_ref), wg_ref[...]).astype(bf16).astype(f32) + dot_nt(natural(du_ref), wu_ref[...]).astype(bf16).astype(f32)
        da = da.astype(bf16).astype(f32)
        wide = h_ref[...].astype(f32)
        scale = scale_of(wide)
        along = jnp.sum(da * wide, -1, keepdims=True) * (scale * scale * scale * (1.0 / D))
        dh = (da * scale - wide * along).astype(bf16)
        out_ref[...] = (dy_ref[...].astype(f32) + dh.astype(f32)).astype(bf16)

        for p in range(3):
            for at, what in ((1 + p, sums.over_x), (5 + 2 * p, sums.over_y), (9 + 2 * p, sums.finish), (15, sums.flushed)):

                @pl.when(t == at)
                def _(what=what, p=p):
                    what(NC - 1, p)

        @pl.when(t == steps - 1)
        def _():
            sq_ref[...] = sums.total()

    row = lambda n: pl.BlockSpec((TB, n), lambda t: (t, 0))
    once = pl.BlockSpec((D, FF), lambda t: (0, 0), pipeline_mode=pl.Buffered(1))
    return pl.pallas_call(
        body,
        grid=(steps,),
        in_specs=[row(FF)] * 2 + [once] * 2 + [row(D)] * 2 + [ANY] * 4,
        out_specs=[row(D)] + [ANY] * 3 + [SQUARES_SPEC],
        out_shape=[sds((TOK, D))] + BLOCKS + [SQUARES],
        input_output_aliases={7: 1, 8: 2, 9: 3},
        scratch_shapes=[DMA] + Summing.SHAPES,
        compiler_params=params(2),
        cost_estimate=cost(2, FF, 80_000_000),
        name="backward_through",
    )(dg, du, wg, wu, h, dy, sk, og, ou, od)


def backward_bottom(a, dy, gate, up, wd):
    def body(a_ref, dy_ref, *rest):
        gate_ref, up_ref, wd_ref = rest[:3]
        og, ou, od, sq_ref, a_v, dy_v, dg_s, du_s, hid_s, sems, *comm = rest[3:]
        j, t = pl.program_id(0), pl.program_id(1)
        sums = Summing(comm, (og, ou, od))
        load_tiles(j, t, ((a_ref, a_v), (dy_ref, dy_v)), sems)

        @pl.when((j == 0) & (t == 0))
        def _():
            sums.meet()

        @pl.when(t < NT)
        def _():
            wdc = wd_ref[...].reshape(CH, D)
            for n in range(TM // SUB):
                r = pl.ds(pl.multiple_of(t * TM + n * SUB, SUB), SUB)
                rr = slice(n * SUB, (n + 1) * SUB)
                g, u = gate_ref[0, rr, :], up_ref[0, rr, :]
                dh = dot_nt(dy_v[r, :], wdc).astype(bf16).astype(f32)
                sig = sigmoid(g)
                silu = g * sig
                dg_s[r, :] = (dh * u * (sig + silu - silu * sig)).astype(bf16)
                du_s[r, :] = (dh * silu).astype(bf16)
                hid_s[r, :] = (silu * u).astype(bf16)

        products(j, t, NC - 1, a_v, dy_v, dg_s, du_s, hid_s, sums)

        @pl.when((j == NC - 1) & (t == NT + 2))
        def _():
            e = NC - 1
            sums.finish(e - 1, 2)
            sums.over_y(e, 0)
            sums.over_x(e, 2)
            sums.over_y(e, 1)
            sums.flushed(e - 1, 2)
            sums.finish(e, 0)
            sums.over_y(e, 2)
            sums.finish(e, 1)
            sums.finish(e, 2)
            for p in range(3):
                sums.flushed(e, p)
            sq_ref[...] = sums.total()

    tile = pl.BlockSpec((1, TM, CH), lambda j, t: (j, jnp.minimum(t, NT - 1), 0))
    return pl.pallas_call(
        body,
        grid=(NC, NT + 3),
        in_specs=[ANY] * 2 + [tile] * 2 + [pl.BlockSpec((4, 128, D), lambda j, t: (0, j, 0))],
        out_specs=[ANY] * 3 + [SQUARES_SPEC],
        out_shape=BLOCKS + [SQUARES],
        scratch_shapes=BACKWARD + Summing.SHAPES,
        compiler_params=params(3),
        cost_estimate=cost(4, FF, 120_000_000),
        name="backward_bottom",
    )(a, dy, gate, up, wd.reshape(4, 640, D))


def adamw(factor, weights, m, v, g0, g1):
    parts = 4

    def body(factor_ref, *refs):
        w, m, v, g0, g1, nw, nm, nv = (refs[3 * n : 3 * n + 3] for n in range(8))
        factor = factor_ref[0]

        def update(g, k):
            g = g[...].astype(f32) * factor
            new_m = 0.9 * m[k][0] + 0.1 * g
            new_v = 0.95 * v[k][0] + 0.05 * g * g
            move = new_m * lax.rsqrt(new_v + 1e-8) + 0.1 * w[k][0].astype(f32)
            nm[k][0] = new_m
            nv[k][0] = new_v
            nw[k][0] = (w[k][0].astype(f32) - 0.02 * move).astype(bf16)

        for n, g in enumerate((g0, g1)):

            @pl.when(pl.program_id(0) == n)
            def _(g=g):
                for k in range(3):
                    update(g[k], k)

    shapes = [(256 // parts, FF)] * 2 + [(640 // parts, D)]
    whole = [pl.BlockSpec((1, *s), lambda n, t: (n, t, 0)) for s in shapes]
    low = [pl.BlockSpec(s, lambda n, t: (jnp.where(n == 0, t, parts - 1), 0)) for s in shapes]
    high = [pl.BlockSpec(s, lambda n, t: (jnp.where(n == 1, t, 0), 0)) for s in shapes]
    return pl.pallas_call(
        body,
        grid=(2, parts),
        in_specs=[pl.BlockSpec(memory_space=pltpu.SMEM)] + whole * 3 + low + high,
        out_specs=whole * 3,
        out_shape=[sds(w.shape, d) for d in (bf16, f32, f32) for w in weights],
        compiler_params=params(),
        name="adamw",
    )(factor, *weights, *m, *v, *g0, *g1)


def solution(mesh):
    def step(x, dy, *arrays):
        weights, m, v = (arrays[i : i + 3] for i in (0, 3, 6))
        x, dy = x[0], dy[0]
        wd0, wg1, wu1, wd1_first, a0, gate, up, h, a1 = forward(x, *weights)
        dg, du, *g1, sk, sq1 = backward_top(a1, dy, wg1, wu1, wd1_first, weights[2])
        dh, *g1, sq2 = backward_through(dg, du, wg1, wu1, h, dy, sk, *g1)
        *g0, sq3 = backward_bottom(a0, dh, gate, up, wd0)
        squares = lax.psum(jnp.sum(sq1 + sq2 + sq3), "s")
        count = lax.psum(1, "s") * sum(w.size for w in weights)
        factor = jnp.minimum(1.0, 0.5 * lax.rsqrt(squares / count + 1e-30))
        return tuple(adamw(factor.reshape(1), weights, m, v, g0, g1))

    states, cut = P(("rep", "r", "s"), None, None), P(None, "s", None)
    return jax.shard_map(
        step,
        mesh=mesh,
        in_specs=(states, states) + (cut,) * 9,
        out_specs=(P("rep", "s", None),) * 9,
        check_vma=False,
    )
```

```python
import jax
import jax.numpy as jnp
from jax import lax
from jax.experimental import pallas as pl
from jax.experimental.pallas import tpu as pltpu
from jax.sharding import PartitionSpec as P

TOK, D, FF = 4096, 1024, 2560
NC, CH = 5, 512
TM, SUB = 1024, 256
ROWS, LANES, QUARTER = 256, 128, 640
THREE, FOUR = range(3), range(4)
NT = TOK // TM
FM, FT = 512, 8
bf16, f32 = jnp.bfloat16, jnp.float32
MESH = pl.DeviceIdType.MESH
ANY = pl.BlockSpec(memory_space=pl.ANY)
VMEM, DMA = pltpu.VMEM, pltpu.SemaphoreType.DMA


def sds(shape, dtype=bf16):
    return jax.ShapeDtypeStruct(shape, dtype)


def params(collective_id=None):
    return pltpu.CompilerParams(vmem_limit_bytes=63 * 1024 * 1024, collective_id=collective_id, has_side_effects=collective_id is not None)


def dot(a, b):
    return jnp.dot(a, b, preferred_element_type=f32)


def dot_nt(a, b):
    return lax.dot_general(a, b, (((1,), (1,)), ((), ())), preferred_element_type=f32)


def dot_tn(a, b):
    return lax.dot_general(a, b, (((0,), (0,)), ((), ())), preferred_element_type=f32)


def cost(products, width, nbytes):
    return pl.CostEstimate(flops=products * 2 * TOK * D * width, bytes_accessed=nbytes, transcendentals=0)


def scale_of(wide):
    return lax.rsqrt(jnp.mean(wide * wide, -1, keepdims=True) + 1e-6)


def sigmoid(g):
    return 0.5 * jnp.tanh(0.5 * g) + 0.5


def places():
    s, r = lax.axis_index("s"), lax.axis_index("r")
    xx, core = s // 2, s % 2
    return s, xx, core, r, {"s": s + 1 - 2 * core}, {"s": s + 2 - 4 * xx}, {"r": 1 - r}


def meet(*others):
    barrier = pltpu.get_barrier_semaphore()
    for other in others:
        pl.semaphore_signal(barrier, inc=1, device_id=other, device_id_type=MESH)
    pl.semaphore_wait(barrier, len(others))


def remote(src, dst, send, recv, other):
    return pltpu.make_async_remote_copy(src_ref=src, dst_ref=dst, send_sem=send, recv_sem=recv, device_id=other, device_id_type=MESH)


UNITS = 14


class Routes:
    def __init__(self, place, mine, send, recv):
        self.place, self.mine, self.send, self.recv = place, mine, send, recv
        self.s, xx, core, self.r, self.mate, self.along_x, self.along_y = places()
        self.near = self.s + 1 - 2 * core
        self.far, self.diag = self.s + 2 - 4 * xx, self.near + 2 - 4 * xx

    def copy(self, kind, k):
        s, r, far = self.s, self.r, self.far
        src, dst, to = (
            lambda: (self.mine(k), self.place(k, s), self.mate),
            lambda: (self.mine(k, r), self.place(k, s, r), self.along_x),
            lambda: (self.place(k, far, r), self.place(k, far, r), self.along_y),
            lambda: (self.place(k, far, r), self.place(k, far, r), self.mate),
            lambda: (self.place(k, far, 1 - r), self.place(k, far, 1 - r), self.mate),
        )[kind]()
        return remote(src, dst, self.send.at[kind, k], self.recv.at[kind, k], to)

    def to_mate(self, k):
        self.copy(0, k).start()

    def to_x(self, k):
        self.copy(1, k).start()

    def got(self, kind, k):
        r = self.r
        here = self.place(k, *((self.near, None), (self.far, r), (self.far, 1 - r), (self.diag, r), (self.diag, 1 - r))[kind])
        remote(here, here, self.send.at[kind, k], self.recv.at[kind, k], self.mate).wait_recv()

    def pass_x(self, k):
        self.got(1, k)
        self.copy(2, k).start()
        self.copy(3, k).start()

    def pass_y(self, k):
        self.got(2, k)
        self.copy(4, k).start()

    def complete(self, k):
        for kind in (0, 3, 4):
            self.got(kind, k)

    def sent(self, k):
        for kind in range(5):
            self.copy(kind, k).wait_send()


def forward(x, wg, wu, wd):
    def body(x_ref, wg_ref, wu_ref, wd_ref, xt_ref, wd0, wg1, wu1, wd1, a0_ref, g_ref, u_ref, h_ref, a1_ref, a_v, wg0, wu0, wd_v, hid_v, st_g, st_u, st_d, st_c, send, recv, local):
        i = pl.program_id(0)
        s = lax.axis_index("s")
        full = (wg0, wu0) * NC + (wd0, wg1, wu1, wd1)
        blocks = (None,) * (2 * NC) + (wd_ref.at[0], wg_ref.at[1], wu_ref.at[1], wd_ref.at[1])

        def size(k):
            return QUARTER if k == 10 else LANES if k == 13 else ROWS

        def place(k, owner, half=None):
            rows = size(k)
            first, count = (0, rows) if half is None else (pl.multiple_of(half * (rows // 2), 64), rows // 2)
            if k == 13:
                return full[k].at[owner, pl.ds(first, count)]
            at = pl.ds(pl.multiple_of(owner * rows + first, 64), count)
            return full[k].at[k // 2, at] if k < 2 * NC else full[k].at[at]

        def mine(k, half=None):
            if k < 2 * NC:
                return place(k, s, half)
            rows = size(k)
            return blocks[k].at[pl.ds(0, rows) if half is None else pl.ds(pl.multiple_of(half * (rows // 2), 64), rows // 2)]

        routes = Routes(place, mine, send, recv)
        x_in = lambda t: pltpu.make_async_copy(x_ref.at[pl.ds(t * FM, FM)], a_v.at[pl.ds(t * FM, FM)], local.at[t])
        a_out = pltpu.make_async_copy(a_v, a0_ref, local.at[8])
        own_in = [pltpu.make_async_copy(m.at[0], st, local.at[9 + n]) for n, (m, st) in enumerate(((wg_ref, st_g), (wu_ref, st_u)))]
        stage = [
            (pltpu.make_async_copy(mine(k), buf, local.at[11 + n]), pltpu.make_async_copy(buf, place(k, s), local.at[15 + n]))
            for n, (k, buf) in enumerate(((10, st_d), (11, st_g), (12, st_u), (13, st_c)))
        ]
        wd_in = pltpu.make_async_copy(wd0, wd_v, local.at[19])

        @pl.when(i == 0)
        def _():
            for c in own_in:
                c.start()
            for t in range(FT):
                x_in(t).start()
            rows = pl.ds(pl.multiple_of(s * ROWS, ROWS), ROWS)
            for c, st, w in zip(own_in, (st_g, st_u), (wg0, wu0)):
                c.wait()
                for j in range(NC):
                    for q in FOUR:
                        w[j, rows, LANES * q : LANES * q + LANES] = st[:, QUARTER * q + LANES * j : QUARTER * q + LANES * j + LANES]
            meet(routes.mate, routes.along_x, routes.along_y)
            for k in range(UNITS):
                routes.to_x(k)
            for k in range(2 * NC):
                routes.to_mate(k)
            for c, _ in stage:
                c.start()

            def norm(t, _):
                x_in(t).wait()
                for n in range(FM // SUB):
                    rows = pl.ds(pl.multiple_of(t * FM + n * SUB, SUB), SUB)
                    wide = a_v[rows, :].astype(f32)
                    a_v[rows, :] = (wide * scale_of(wide)).astype(bf16)
                return 0

            lax.fori_loop(0, FT, norm, 0)
            routes.pass_x(0)
            routes.pass_x(1)
            a_out.start()
            for k in range(2 * NC, UNITS):
                routes.to_mate(k)
            for c, d in stage:
                c.wait()
                d.start()
            for k in (2, 3):
                routes.pass_x(k)
            for k in (0, 1):
                routes.pass_y(k)

        for c in range(NC):

            @pl.when(i == c * FT)
            def _(c=c):
                routes.complete(2 * c)
                routes.complete(2 * c + 1)

        events = [(FT // 2, "y", 2), (FT // 2, "y", 3)]
        for k in range(4, 2 * NC):
            at = (k // 2 - 2) * (FT - 3) + 3
            events += [(at, "x", k), (at + 1 + FT // 2 if k < 8 else at + FT // 2, "y", k)]
        events += [(23, "x", 10), (23 + 9, "x", 11), (23 + 11, "y", 10), (23 + 18, "x", 12), (23 + 18, "y", 11), (23 + 19, "x", 13)]

        def event(which, k):
            (routes.pass_x if which == "x" else routes.pass_y)(k)

        for c in range(NC):

            @pl.when(i // FT == c)
            def _(c=c):
                for n in range(FM // SUB):
                    rows = pl.ds(pl.multiple_of(i % FT * FM + n * SUB, SUB), SUB)
                    a = a_v[rows, :]
                    g, u = dot(a, wg0[c]), dot(a, wu0[c])
                    g_ref[0, n * SUB : (n + 1) * SUB, :] = g
                    u_ref[0, n * SUB : (n + 1) * SUB, :] = u
                    hid = (g * sigmoid(g) * u).astype(bf16)
                    for q in FOUR:
                        hid_v[rows, QUARTER * q + LANES * c : QUARTER * q + LANES * c + LANES] = hid[:, LANES * q : LANES * q + LANES]

        @pl.when(i == NC * FT)
        def _():
            routes.complete(10)
            stage[0][1].wait()
            wd_in.start()
            wd_in.wait()

        @pl.when(i >= NC * FT)
        def _():
            rows = pl.ds(pl.multiple_of(i % FT * FM, FM), FM)
            y = dot(hid_v[rows, :], wd_v[...]).astype(bf16)
            h = (xt_ref[...].astype(f32) + y.astype(f32)).astype(bf16)
            h_ref[...] = h
            wide = h.astype(f32)
            a1_ref[...] = (wide * scale_of(wide)).astype(bf16)

        for at in sorted({e[0] for e in events}):

            @pl.when(i == at)
            def _(at=at):
                for e in events:
                    if e[0] == at:
                        event(*e[1:])

        @pl.when(i == NC * FT + FT - 1)
        def _():
            routes.pass_y(12)
            routes.pass_y(13)
            for k in (11, 12, 13):
                routes.complete(k)
            for k in range(UNITS):
                routes.sent(k)
            for _, d in stage[1:]:
                d.wait()
            a_out.wait()

    late = lambda i: (jnp.maximum(i - NC * FT, 0), 0)
    tile = lambda i: (jnp.minimum(i // FT, NC - 1), jnp.where(i < NC * FT, i % FT, FT - 1), 0)
    return pl.pallas_call(
        body,
        grid=(NC * FT + FT,),
        in_specs=[ANY] * 4 + [pl.BlockSpec((FM, D), late)],
        out_specs=[ANY] * 5 + [pl.BlockSpec((1, FM, CH), tile)] * 2 + [pl.BlockSpec((FM, D), late)] * 2,
        out_shape=[sds((FF, D)), sds((D, FF)), sds((D, FF)), sds((4, LANES, D)), sds((TOK, D)), sds((NC, TOK, CH), f32), sds((NC, TOK, CH), f32), sds((TOK, D)), sds((TOK, D))],
        scratch_shapes=[
            VMEM((TOK, D), bf16),
            VMEM((NC, D, CH), bf16),
            VMEM((NC, D, CH), bf16),
            VMEM((FF, D), bf16),
            VMEM((TOK, FF), bf16),
            VMEM((ROWS, FF), bf16),
            VMEM((ROWS, FF), bf16),
            VMEM((QUARTER, D), bf16),
            VMEM((LANES, D), bf16),
            DMA((5, UNITS)),
            DMA((5, UNITS)),
            DMA((20,)),
        ],
        compiler_params=params(0),
        cost_estimate=cost(3, FF, 150_000_000),
        name="forward",
    )(x, wg, wu, wd, x)


class Summing:
    SHAPES = [
        VMEM((3, 2, 2, ROWS, CH), bf16),
        VMEM((2, 3, 2, ROWS, CH), bf16),
        VMEM((2, 3, ROWS, CH), bf16),
        VMEM((2, 3, ROWS, CH), bf16),
        VMEM((3, ROWS, CH), bf16),
        VMEM((3, ROWS, CH), bf16),
        VMEM((ROWS, CH), f32),
        DMA((3, 2, 3)),
        DMA((3, 2, 3)),
        DMA((3, 4)),
    ]

    def __init__(self, refs, outs):
        self.sk, self.r1, self.r2, self.r3, self.ours, self.fin, self.squares, self.send, self.recv, self.local = refs
        self.outs = outs
        _, self.xx, self.core, _, self.mate, self.along_x, self.along_y = places()

    def meet(self):
        meet(self.mate, self.along_x, self.along_y)
        self.squares[...] = jnp.zeros_like(self.squares)

    def where(self, o):
        return self.core if o % 2 else 1 - self.core, self.xx if o // 2 else 1 - self.xx

    def put(self, p, a, b):
        for n in range(4 if p < 2 else 2):
            value = dot_tn(a[:, ROWS * n : ROWS * n + ROWS], b[...]).astype(bf16)
            if p < 2:
                kc, kx = self.where(n)
                self.sk[p, kc, kx] = value
                continue
            for o in (0, 1):
                kc, kx = self.where(2 * n + o)
                for q in (0, 1):
                    self.sk[p, kc, kx, LANES * q : LANES * q + LANES] = value[LANES * o : LANES * o + LANES, CH * q : CH * q + CH]

    def copy(self, stage, j, p):
        b = j % 2
        src, dst, to = (
            (self.sk.at[p, 0], self.r1.at[b, p], self.mate),
            (self.sk.at[p, 1, 0], self.r2.at[b, p], self.along_x),
            (self.ours.at[p], self.r3.at[b, p], self.along_y),
        )[stage]
        return remote(src, dst, self.send.at[stage, b, p], self.recv.at[stage, b, p], to)

    def start(self, j, p):
        self.copy(0, j, p).start()

    def over_x(self, j, p):
        self.copy(0, j, p).wait()
        self.sk[p, 1, 0] = (self.sk[p, 1, 0].astype(f32) + self.r1[j % 2, p, 0].astype(f32)).astype(bf16)
        self.copy(1, j, p).start()

    def over_y(self, j, p):
        self.copy(1, j, p).wait()
        b = j % 2
        self.ours[p] = (self.sk[p, 1, 1].astype(f32) + self.r1[b, p, 1].astype(f32) + self.r2[b, p].astype(f32)).astype(bf16)
        self.copy(2, j, p).start()

    def out(self, j, p):
        if p < 2:
            return [
                pltpu.make_async_copy(
                    self.fin.at[p, :, pl.ds(LANES * q, LANES)], self.outs[p].at[:, pl.ds(pl.multiple_of(QUARTER * q + LANES * j, LANES), LANES)], self.local.at[p, q]
                )
                for q in FOUR
            ]
        rows = pl.ds(pl.multiple_of(LANES * j, LANES), LANES)
        return [pltpu.make_async_copy(self.fin.at[p, pl.ds(LANES * q, LANES)], self.outs[p].at[rows, pl.ds(CH * q, CH)], self.local.at[p, q]) for q in range(2)]

    def finish(self, j, p):
        self.copy(2, j, p).wait()
        g = (self.ours[p].astype(f32) + self.r3[j % 2, p].astype(f32)).astype(bf16)
        self.fin[p] = g
        g = g.astype(f32)
        self.squares[...] += g * g
        for c in self.out(j, p):
            c.start()

    def total(self):
        return sum(self.squares[8 * n : 8 * n + 8, :] for n in range(32))

    def flushed(self, j, p):
        for c in self.out(j, p):
            c.wait()

    def beside(self, j, t, steps):
        for at, what in (
            (1, lambda: (self.over_y(j - 1, 0), self.over_x(j - 1, 2))),
            (NT, lambda: (self.over_y(j - 1, 1), self.finish(j - 1, 0))),
            (NT + 1, lambda: self.over_y(j - 1, 2)),
            (NT + 2, lambda: (self.finish(j - 1, 1), self.flushed(j - 1, 0), self.flushed(j - 1, 1))),
        ):
            if at in steps:

                @pl.when((j >= 1) & (t == at))
                def _(what=what):
                    what()

        if 2 in steps:

            @pl.when((j >= 2) & (t == 2))
            def _():
                self.finish(j - 2, 2)

            @pl.when((j >= 2) & (t == 3))
            def _():
                self.flushed(j - 2, 2)


def products(j, t, last, a_v, dy_v, dg_s, du_s, hid_s, sums):
    sums.beside(j, t, range(NT))

    @pl.when(t == NT)
    def _():
        sums.put(0, a_v, dg_s)
        sums.beside(j, t, [NT])

        @pl.when(j <= last)
        def _():
            sums.start(j, 0)

    @pl.when(t == NT + 1)
    def _():
        sums.put(1, a_v, du_s)
        sums.beside(j, t, [NT + 1])

        @pl.when(j <= last)
        def _():
            sums.over_x(j, 0)
            sums.start(j, 1)

    @pl.when(t == NT + 2)
    def _():
        sums.put(2, hid_s, dy_v)
        sums.beside(j, t, [NT + 2])

        @pl.when(j <= last)
        def _():
            sums.over_x(j, 1)
            sums.start(j, 2)


def load_tiles(j, t, pairs, sems):
    rows = lambda i: pl.ds(pl.multiple_of(i * TM, TM), TM)
    copies = lambda i: [pltpu.make_async_copy(src.at[rows(i)], dst.at[rows(i)], sems.at[n, i]) for n, (src, dst) in enumerate(pairs)]

    @pl.when((j == 0) & (t == 0))
    def _():
        for i in range(NT):
            for c in copies(i):
                c.start()

    @pl.when((j == 0) & (t < NT))
    def _():
        for c in copies(t):
            c.wait()


BACKWARD = [VMEM((TOK, D), bf16)] * 2 + [VMEM((TOK, CH), bf16)] * 3 + [DMA((2, NT))]
BLOCKS = [sds((ROWS, FF)), sds((ROWS, FF)), sds((QUARTER, D))]
SQUARES = sds((8, CH), f32)
SQUARES_SPEC = pl.BlockSpec((8, CH), lambda *_: (0, 0))


def backward_top(a, dy, wg, wu, wd_first, wd):
    def body(a_ref, dy_ref, *rest):
        wgs, wus, first_ref, wd_ref = rest[0:4], rest[4:8], rest[8], rest[9]
        dg_ref, du_ref, og, ou, od, sk_ref, sq_ref, a_v, dy_v, dg_s, du_s, hid_s, sems, wgc, wuc, last_sem, wd_v, send, recv, own_sem, *comm = rest[10:]
        j, t = pl.program_id(0), pl.program_id(1)
        sums = Summing(comm, (og, ou, od))
        load_tiles(j, t, ((a_ref, a_v), (dy_ref, dy_v)), sems)

        s = lax.axis_index("s")
        rows = lambda half: pl.ds(0, LANES) if half is None else pl.ds(pl.multiple_of(64 * half, 64), 64)
        routes = Routes(
            lambda k, owner, half=None: wd_v.at[k, owner, rows(half)],
            lambda k, half=None: wd_v.at[k, s, rows(half)],
            send,
            recv,
        )
        own = [pltpu.make_async_copy(wd_ref.at[1, pl.ds(LANES * k, LANES)] if k else first_ref, wd_v.at[k, s] if k else wd_v.at[0], own_sem.at[k]) for k in range(NC)]
        later = range(1, NC)

        @pl.when((j == 0) & (t == 0))
        def _():
            for c in own:
                c.start()
            sums.meet()
            for c in own:
                c.wait()
            for k in later:
                routes.to_x(k)
            for k in later:
                routes.to_mate(k)

        @pl.when((j == 0) & (t == 3))
        def _():
            for k in later:
                routes.pass_x(k)

        @pl.when((j == 0) & (t == NT + 1))
        def _():
            for k in later:
                routes.pass_y(k)

        for k in later:

            @pl.when((j == k) & (t == 0))
            def _(k=k):
                routes.complete(k)

        @pl.when(t == 0)
        def _():
            wgc[...] = jnp.concatenate([w[...] for w in wgs], axis=1)
            wuc[...] = jnp.concatenate([w[...] for w in wus], axis=1)

        @pl.when(t < NT)
        def _():
            wdc = wd_v[j].reshape(CH, D)
            for n in range(TM // SUB):
                r = pl.ds(pl.multiple_of(t * TM + n * SUB, SUB), SUB)
                x = a_v[r, :]
                g, u = dot(x, wgc[...]), dot(x, wuc[...])
                dh = dot_nt(dy_v[r, :], wdc).astype(bf16).astype(f32)
                sig = sigmoid(g)
                silu = g * sig
                dg = (dh * u * (sig + silu - silu * sig)).astype(bf16)
                du = (dh * silu).astype(bf16)
                hid_s[r, :] = (silu * u).astype(bf16)
                dg_s[r, :] = dg
                du_s[r, :] = du
                dg_ref[n * SUB : (n + 1) * SUB, :] = dg
                du_ref[n * SUB : (n + 1) * SUB, :] = du

        products(j, t, NC - 2, a_v, dy_v, dg_s, du_s, hid_s, sums)

        @pl.when((j == NC - 1) & (t == NT + 2))
        def _():
            give = pltpu.make_async_copy(sums.sk, sk_ref, last_sem)
            give.start()
            sums.finish(NC - 2, 2)
            sums.flushed(NC - 2, 2)
            sq_ref[...] = sums.total()
            for k in later:
                routes.sent(k)
            give.wait()

    col = [pl.BlockSpec((D, LANES), lambda j, t, q=q: (0, q * NC + j)) for q in FOUR]
    tile = pl.BlockSpec((TM, CH), lambda j, t: (jnp.minimum(t, NT - 1), j))
    return pl.pallas_call(
        body,
        grid=(NC, NT + 3),
        in_specs=[ANY] * 2 + col + col + [ANY] * 2,
        out_specs=[tile, tile] + [ANY] * 4 + [SQUARES_SPEC],
        out_shape=[sds((TOK, FF))] * 2 + BLOCKS + [sds((3, 2, 2, ROWS, CH)), SQUARES],
        scratch_shapes=BACKWARD + [VMEM((D, CH), bf16)] * 2 + [DMA, VMEM((NC, 4, LANES, D), bf16), DMA((5, NC)), DMA((5, NC)), DMA((NC,))] + Summing.SHAPES,
        compiler_params=params(1),
        cost_estimate=cost(6, FF, 80_000_000),
        name="backward_top",
    )(a, dy, *[wg] * 4, *[wu] * 4, wd_first, wd)


def backward_through(dg, du, wg, wu, h, dy, sk, og, ou, od):
    TB = ROWS
    steps = TOK // TB

    def body(dg_ref, du_ref, wg_ref, wu_ref, h_ref, dy_ref, sk_ref, _a, _b, _c, out_ref, og, ou, od, sq_ref, sem, *comm):
        t = pl.program_id(0)
        sums = Summing(comm, (og, ou, od))

        @pl.when(t == 0)
        def _():
            take = pltpu.make_async_copy(sk_ref, sums.sk, sem)
            take.start()
            sums.meet()
            take.wait()
            for p in THREE:
                sums.start(NC - 1, p)

        natural = lambda ref: jnp.concatenate([ref[:, CH * j + LANES * q : CH * j + LANES * q + LANES] for q in FOUR for j in range(NC)], axis=1)
        da = dot_nt(natural(dg_ref), wg_ref[...]).astype(bf16).astype(f32) + dot_nt(natural(du_ref), wu_ref[...]).astype(bf16).astype(f32)
        da = da.astype(bf16).astype(f32)
        wide = h_ref[...].astype(f32)
        scale = scale_of(wide)
        along = jnp.sum(da * wide, -1, keepdims=True) * (scale * scale * scale * (1.0 / D))
        dh = (da * scale - wide * along).astype(bf16)
        out_ref[...] = (dy_ref[...].astype(f32) + dh.astype(f32)).astype(bf16)

        for p in THREE:
            for at, what in ((1 + p, sums.over_x), (5 + 2 * p, sums.over_y), (9 + 2 * p, sums.finish), (15, sums.flushed)):

                @pl.when(t == at)
                def _(what=what, p=p):
                    what(NC - 1, p)

        @pl.when(t == steps - 1)
        def _():
            sq_ref[...] = sums.total()

    row = lambda n: pl.BlockSpec((TB, n), lambda t: (t, 0))
    once = pl.BlockSpec((D, FF), lambda t: (0, 0), pipeline_mode=pl.Buffered(1))
    return pl.pallas_call(
        body,
        grid=(steps,),
        in_specs=[row(FF)] * 2 + [once] * 2 + [row(D)] * 2 + [ANY] * 4,
        out_specs=[row(D)] + [ANY] * 3 + [SQUARES_SPEC],
        out_shape=[sds((TOK, D))] + BLOCKS + [SQUARES],
        input_output_aliases={7: 1, 8: 2, 9: 3},
        scratch_shapes=[DMA] + Summing.SHAPES,
        compiler_params=params(2),
        cost_estimate=cost(2, FF, 80_000_000),
        name="backward_through",
    )(dg, du, wg, wu, h, dy, sk, og, ou, od)


def backward_bottom(a, dy, gate, up, wd):
    def body(a_ref, dy_ref, *rest):
        gate_ref, up_ref, wd_ref = rest[:3]
        og, ou, od, sq_ref, a_v, dy_v, dg_s, du_s, hid_s, sems, *comm = rest[3:]
        j, t = pl.program_id(0), pl.program_id(1)
        sums = Summing(comm, (og, ou, od))
        load_tiles(j, t, ((a_ref, a_v), (dy_ref, dy_v)), sems)

        @pl.when((j == 0) & (t == 0))
        def _():
            sums.meet()

        @pl.when(t < NT)
        def _():
            wdc = wd_ref[...].reshape(CH, D)
            for n in range(TM // SUB):
                r = pl.ds(pl.multiple_of(t * TM + n * SUB, SUB), SUB)
                rr = slice(n * SUB, (n + 1) * SUB)
                g, u = gate_ref[0, rr, :], up_ref[0, rr, :]
                dh = dot_nt(dy_v[r, :], wdc).astype(bf16).astype(f32)
                sig = sigmoid(g)
                silu = g * sig
                dg_s[r, :] = (dh * u * (sig + silu - silu * sig)).astype(bf16)
                du_s[r, :] = (dh * silu).astype(bf16)
                hid_s[r, :] = (silu * u).astype(bf16)

        products(j, t, NC - 1, a_v, dy_v, dg_s, du_s, hid_s, sums)

        @pl.when((j == NC - 1) & (t == NT + 2))
        def _():
            e = NC - 1
            sums.finish(e - 1, 2)
            sums.over_y(e, 0)
            sums.over_x(e, 2)
            sums.over_y(e, 1)
            sums.flushed(e - 1, 2)
            sums.finish(e, 0)
            sums.over_y(e, 2)
            sums.finish(e, 1)
            sums.finish(e, 2)
            for p in THREE:
                sums.flushed(e, p)
            sq_ref[...] = sums.total()

    tile = pl.BlockSpec((1, TM, CH), lambda j, t: (j, jnp.minimum(t, NT - 1), 0))
    return pl.pallas_call(
        body,
        grid=(NC, NT + 3),
        in_specs=[ANY] * 2 + [tile] * 2 + [pl.BlockSpec((4, LANES, D), lambda j, t: (0, j, 0))],
        out_specs=[ANY] * 3 + [SQUARES_SPEC],
        out_shape=BLOCKS + [SQUARES],
        scratch_shapes=BACKWARD + Summing.SHAPES,
        compiler_params=params(3),
        cost_estimate=cost(4, FF, 120_000_000),
        name="backward_bottom",
    )(a, dy, gate, up, wd.reshape(4, QUARTER, D))


def adamw(factor, weights, m, v, g0, g1):
    parts = 4

    def body(factor_ref, *refs):
        w, m, v, g0, g1, nw, nm, nv = (refs[3 * n : 3 * n + 3] for n in range(8))
        factor = factor_ref[0]

        def update(g, k):
            g = g[...].astype(f32) * factor
            new_m = 0.9 * m[k][0] + 0.1 * g
            new_v = 0.95 * v[k][0] + 0.05 * g * g
            move = new_m * lax.rsqrt(new_v + 1e-8) + 0.1 * w[k][0].astype(f32)
            nm[k][0] = new_m
            nv[k][0] = new_v
            nw[k][0] = (w[k][0].astype(f32) - 0.02 * move).astype(bf16)

        for n, g in enumerate((g0, g1)):

            @pl.when(pl.program_id(0) == n)
            def _(g=g):
                for k in THREE:
                    update(g[k], k)

    shapes = [(ROWS // parts, FF)] * 2 + [(QUARTER // parts, D)]
    whole = [pl.BlockSpec((1, *s), lambda n, t: (n, t, 0)) for s in shapes]
    low = [pl.BlockSpec(s, lambda n, t: (jnp.where(n == 0, t, parts - 1), 0)) for s in shapes]
    high = [pl.BlockSpec(s, lambda n, t: (jnp.where(n == 1, t, 0), 0)) for s in shapes]
    return pl.pallas_call(
        body,
        grid=(2, parts),
        in_specs=[pl.BlockSpec(memory_space=pltpu.SMEM)] + whole * 3 + low + high,
        out_specs=whole * 3,
        out_shape=[sds(w.shape, d) for d in (bf16, f32, f32) for w in weights],
        compiler_params=params(),
        name="adamw",
    )(factor, *weights, *m, *v, *g0, *g1)


def solution(mesh):
    def step(x, dy, *arrays):
        weights, m, v = (arrays[i : i + 3] for i in (0, 3, 6))
        x, dy = x[0], dy[0]
        wd0, wg1, wu1, wd1_first, a0, gate, up, h, a1 = forward(x, *weights)
        dg, du, *g1, sk, sq1 = backward_top(a1, dy, wg1, wu1, wd1_first, weights[2])
        dh, *g1, sq2 = backward_through(dg, du, wg1, wu1, h, dy, sk, *g1)
        *g0, sq3 = backward_bottom(a0, dh, gate, up, wd0)
        squares = lax.psum(jnp.sum(sq1 + sq2 + sq3), "s")
        count = lax.psum(1, "s") * sum(w.size for w in weights)
        factor = jnp.minimum(1.0, 0.5 * lax.rsqrt(squares / count + 1e-30))
        return tuple(adamw(factor.reshape(1), weights, m, v, g0, g1))

    states, cut = P(("rep", "r", "s"), None, None), P(None, "s", None)
    return jax.shard_map(
        step,
        mesh=mesh,
        in_specs=(states, states) + (cut,) * 9,
        out_specs=(P("rep", "s", None),) * 9,
        check_vma=False,
    )
```
